32 devices in a mesh: gz: 4 (over y, x), gy: 8 (over z, core).
Axes of the slice: x: 2, y: 2, z: 4, core: 2. Of those that a mesh axis runs over, the one named last changes fastest.
Arguments:
- velocity: float32 [3, 32, 128, 768], P(None, 'gz', 'gy'), may hold values from -6 to 6
- forces: bfloat16 [1024, 3, 128], P(('gz', 'gy')), may hold values from -6 to 6
- kernels: bfloat16 [1024, 128, 256], P(('gz', 'gy')), may hold values from -0.5 to 0.5
- owners: int32 [1024, 1], P(('gz', 'gy')), may hold values from 0 to 7; in each aligned block of 32 rows (0 to 31, 32 to 63, ...) at most 8 rows name the same one
- blocks: int32 [1024], P(('gz', 'gy')), may hold values from 0 to 383
- counts: int32 [32], P(('gz', 'gy')), may hold values from 16 to 32, as said below
Outputs:
- velocity_next: float32 [3, 32, 128, 768], P(None, 'gz', 'gy')
- patch_velocity: float32 [1024, 3, 128], P(('gz', 'gy'))
The draws below stay inside these ranges and needn't reach their ends.
Inputs may be any that keep to these rules, and one draw needn't show every extreme that they name: `owners`: owners are gy indices in the holder's own row along gz; among the 32 patches of one device at most 8 share an owner, and some owner has exactly 8. `blocks`: A cell block index within the owner's part of the grid. `counts`: live patches come first in a device's slots; some device has all 32 live.
All inputs are finite; a program needn't handle non-finite values.
Results may differ from the reference program's by a relative error of at most 0.0027.
Values may be sent and summed in bfloat16 or wider, within the bound.
A program may use at most 64 MiB of HBM per device.

```python
import math
import jax
import jax.numpy as jnp
import numpy as np
from jax import lax

CZ = 8
CY = 16
NX = 768
PD = 32
PTS = 128
BLK = 256
NBLK = 384
CAP = 8
NZ = 32
NY = 128
PATCHES = 1024
N_GZ = 4
N_GY = 8


def draw_counts(key, part):
    total = N_GZ * N_GY
    values = jax.random.randint(key, (total,), PD // 2, PD + 1).astype(jnp.int32)
    chosen = jax.random.randint(jax.random.fold_in(key, 7), (), 0, total).astype(jnp.int32)
    return values.at[chosen].set(PD)


def touch_ends(values, key, low, high):
    spot = [jax.random.randint(jax.random.fold_in(key, axis), (), 0, length) for axis, length in enumerate(values.shape)]
    main_axis = values.shape.index(max(values.shape))
    next_to = spot[:main_axis] + [(spot[main_axis] + 1) % values.shape[main_axis]] + spot[main_axis + 1:]
    return values.at[tuple(spot)].set(low).at[tuple(next_to)].set(high)


def shard_levels(stream_key, extent, shards, low, largest):
    gain, own = 1.0, jax.random.fold_in(stream_key, 6)
    for position, shards_of in shards:
        steps = jnp.exp(jax.random.uniform(jax.random.fold_in(own, position), (shards_of,), jnp.float32, low / len(shards), largest / len(shards)))
        gain = gain * jnp.repeat(steps, extent[position] // shards_of).reshape([-1 if axis == position else 1 for axis in range(len(extent))])
    return gain


def deal_out(own_key, own, number, rows, amount, top, bound, lean):
    order = jax.random.permutation(own_key, amount)
    crowded, usual = portions_of(amount, rows * top, bound, lean, True), portions_of(amount, rows * top, bound, lean, False)
    places = jnp.arange(amount)

    def named(lengths, offset_by):
        used = int((lengths > 0).sum())
        fixed = max(1, used // 4)
        moved = fixed + (places - fixed + offset_by * (used - fixed)) % max(1, amount - fixed)
        return jnp.zeros((amount,), jnp.int32).at[order[jnp.where(places < fixed, places, moved)]].set(jnp.asarray(lengths, jnp.int32))

    lengths = jnp.where(number % 4 == 0, named(crowded, number // 4), named(usual, number - number // 4 - 1))
    mixed = jax.random.permutation(jax.random.fold_in(own, 3), amount)
    giver, receiver = mixed[0:amount // 2 * 2:2], mixed[1:amount // 2 * 2:2]
    slack = jnp.minimum(lengths[giver] - 1, bound - lengths[receiver]) // 2
    slack = jnp.where((giver == order[0]) | (receiver == order[0]) | (lengths[receiver] == 0), 0, jnp.maximum(slack, 0))
    moved = jax.random.randint(jax.random.fold_in(own, 4), (amount // 2,), 0, 1 << 20) % (slack + 1)
    lengths = lengths.at[giver].add(-moved).at[receiver].add(moved)
    items = jnp.searchsorted(jnp.cumsum(lengths), jnp.arange(rows * top), side="right").astype(jnp.int32)
    table = items.reshape(top, rows).T
    table = table[jax.random.permutation(jax.random.fold_in(own, 1), rows)]
    offset_by = jax.random.randint(jax.random.fold_in(own, 2), (rows, 1), 0, top)
    return jnp.take_along_axis(table, (jnp.arange(top)[None, :] + offset_by) % top, axis=1)


def portions_of(number_of, total, most, slope, full):
    loads = [(1 << 20) // math.isqrt(standing ** slope) + 1 for standing in range(1, number_of + 1)]
    largest = most if full else min(most, max(-(-total // number_of), total * loads[0] // sum(loads)))
    least = 1 if total - largest >= number_of - 1 else 0
    holding, rest = [largest] + [least] * (number_of - 1), total - largest - least * (number_of - 1)
    while rest > 0:
        movable = [i for i in range(1, number_of) if holding[i] < largest] or [i for i in range(1, number_of) if holding[i] < most]
        whole, remaining = sum([loads[i] for i in movable]), rest
        for i in movable:
            addition = min(most - holding[i], max(1, remaining * loads[i] // whole), rest)
            holding[i] = holding[i] + addition
            rest = rest - addition
    return np.array(holding)


def gaussian(stream_key, shape, scale, reach, cuts=(), held_as=jnp.bfloat16):
    drawn = scale * jax.random.normal(stream_key, shape, jnp.float32)
    if cuts:
        drawn = drawn * shard_levels(stream_key, shape, cuts, -0.22, 0.18)
    return jnp.clip(drawn, -reach, reach).astype(held_as)


def setup_inputs(seed: int = 0) -> dict:
    splits = jax.random.split(jax.random.key(seed), 7)
    velocity = gaussian(splits[0], (3, NZ, NY, NX), 1.0, 6.0, ((1, 4), (2, 8)), jnp.float32)
    forces = gaussian(splits[1], (PATCHES, 3, PTS), 1.0, 6.0, ((0, 32),))
    kernels = gaussian(splits[2], (PATCHES, PTS, BLK), PTS ** -0.5, 0.5, ((0, 32),))
    owners_keys = jax.random.split(jax.random.fold_in(splits[3], 1), PATCHES // PD)
    owners_turns = jax.random.permutation(jax.random.fold_in(splits[3], 3), PATCHES // PD)
    owners = jax.vmap(lambda own, number: deal_out(jax.random.fold_in(splits[3], 2), own, number, PD, N_GY, 1, CAP, 2))(owners_keys, owners_turns).reshape((PATCHES, 1))
    blocks = touch_ends(jax.random.randint(splits[4], (PATCHES,), 0, NBLK), jax.random.fold_in(splits[4], 1), 0, NBLK - 1).astype(jnp.int32)
    counts = draw_counts(jax.random.fold_in(splits[6], 71), 0)
    return dict(velocity=velocity, forces=forces, kernels=kernels, owners=owners, blocks=blocks, counts=counts)


time_step = 0.25
viscosity = 0.5


def reference(velocity, forces, kernels, owners, blocks, counts):
    devices = N_GZ * N_GY
    xblocks = NX // BLK
    forces_dev = forces.reshape(devices, PD, 3, PTS)
    kernels_dev = kernels.reshape(devices, PD, PTS, BLK)
    live = (jnp.arange(PD, dtype=jnp.int32)[None, :] < counts[:, None]).astype(jnp.float32)

    def spread_one(items):
        force_pts, kernel, alive = items
        prod = jnp.einsum("pcq,pqb->pcb", force_pts.astype(jnp.float32), kernel.astype(jnp.float32))
        return (prod * alive[:, None, None]).astype(jnp.bfloat16)

    contribution = lax.map(spread_one, (forces_dev, kernels_dev, live)).reshape(devices * PD, 3, BLK)
    holder_row = ((jnp.arange(devices * PD, dtype=jnp.int32) // PD) // N_GY).astype(jnp.int32)
    owner_col = owners[:, 0].astype(jnp.int32)
    plane = blocks // (CY * xblocks)
    row_in = (blocks // xblocks) % CY
    xblock = blocks % xblocks
    global_id = (((holder_row * CZ + plane) * NY + owner_col * CY + row_in) * xblocks + xblock).astype(jnp.int32)
    force = jax.ops.segment_sum(contribution.astype(jnp.float32), global_id, num_segments=NZ * NY * xblocks)
    force = force.transpose(1, 0, 2).reshape(3, NZ, NY, NX)
    padded = jnp.pad(velocity, ((0, 0), (1, 1), (1, 1), (1, 1)))

    def plane_step(zidx):
        zero = jnp.int32(0)
        window = lax.dynamic_slice(padded, (zero, zidx, zero, zero), (3, 3, NY + 2, NX + 2))
        center = window[:, 1, 1:-1, 1:-1]
        x_up = window[:, 1, 1:-1, 2:]
        x_down = window[:, 1, 1:-1, :-2]
        y_up = window[:, 1, 2:, 1:-1]
        y_down = window[:, 1, :-2, 1:-1]
        z_up = window[:, 2, 1:-1, 1:-1]
        z_down = window[:, 0, 1:-1, 1:-1]
        lap = x_up + x_down + y_up + y_down + z_up + z_down - 6.0 * center
        adv = center[0:1] * (x_up - x_down) * 0.5 + center[1:2] * (y_up - y_down) * 0.5 + center[2:3] * (z_up - z_down) * 0.5
        force_plane = lax.dynamic_index_in_dim(force, zidx, 1, keepdims=False)
        return center + time_step * (viscosity * lap - adv + force_plane)

    fresh = lax.map(plane_step, jnp.arange(NZ, dtype=jnp.int32)).transpose(1, 0, 2, 3)
    cell_blocks = fresh.reshape(3, NZ * NY * xblocks, BLK)

    def sample_one(items):
        ids, kernel, alive = items
        picked = jnp.take(cell_blocks, ids, axis=1).transpose(1, 0, 2).astype(jnp.bfloat16)
        result = jnp.einsum("pcb,pqb->pcq", picked.astype(jnp.float32), kernel.astype(jnp.float32))
        return result * alive[:, None, None]

    sampled = lax.map(sample_one, (global_id.reshape(devices, PD), kernels_dev, live))
    return fresh, sampled.reshape(devices * PD, 3, PTS)
```

```python
import functools

import jax
import jax.numpy as jnp
from jax import lax
from jax.experimental import pallas as pl
from jax.experimental.pallas import tpu as pltpu
from jax.sharding import PartitionSpec as P

time_step = 0.25
vmem_bytes = 67043328
viscosity = 0.5
MESH = pl.DeviceIdType.MESH
f32 = jnp.float32
bf16 = jnp.bfloat16


def iota(shape, dim):
    return lax.broadcasted_iota(jnp.int32, shape, dim)


def step_kernel(width, depth, room, vel_hbm, force_hbm, kern_hbm, own_hbm, blk_hbm, cnt_hbm,
                fresh, kv, held_ref,
                v, force_ref, own_ref, blk_ref, cnt_ref, cells16, left_ref, id_out, id_in, send, recv, back, mine,
                zs, zr, ys, yr,
                in_sem, kern_sem, id_send, id_recv, go_send, go_recv, re_send, re_recv, h_send, h_recv):
    me = lax.axis_index("gy")
    gz = lax.axis_index("gz")
    comps, planes, rows, xcells = v.shape
    _, slots, pts = force_ref.shape
    cells = kv.shape[1]
    nx = xcells // cells
    zy = planes * rows
    total = width * room
    body = comps * cells
    coef = time_step * viscosity
    half = time_step * 0.5
    group = 8
    groups = slots // group
    span = group * pts

    barrier = pltpu.get_barrier_semaphore()
    for k in range(1, width):
        pl.semaphore_signal(barrier, inc=1, device_id={"gy": lax.rem(me + k, width)}, device_id_type=MESH)
    z_lo, z_hi = gz > 0, gz < depth - 1
    y_lo, y_hi = me > 0, me < width - 1

    @pl.when(z_lo)
    def _():
        pl.semaphore_signal(barrier, inc=1, device_id={"gz": gz - 1}, device_id_type=MESH)

    @pl.when(z_hi)
    def _():
        pl.semaphore_signal(barrier, inc=1, device_id={"gz": gz + 1}, device_id_type=MESH)

    gets = [pltpu.make_async_copy(src, dst, in_sem.at[i]) for i, (src, dst) in enumerate((
        (own_hbm, own_ref), (blk_hbm, blk_ref), (cnt_hbm, cnt_ref), (force_hbm, force_ref), (vel_hbm, v)))]
    get_kern = [pltpu.make_async_copy(kern_hbm.at[pl.ds(g * span, span)], kv.at[pl.ds(g * span, span)],
                                      kern_sem.at[g]) for g in range(groups)]
    for copy in gets + get_kern:
        copy.start()

    for copy in gets[:3]:
        copy.wait()
    rowi, coli = iota((slots, slots), 0), iota((slots, slots), 1)
    own_r = jnp.broadcast_to(own_ref[...].astype(f32), (slots, slots))
    own_c = jnp.sum(jnp.where(rowi == coli, own_r, 0.0), axis=1, keepdims=True)
    same = jnp.where(own_r == own_c, 1.0, 0.0)
    rank_c = jnp.sum(jnp.where(coli < rowi, same, 0.0), axis=1, keepdims=True)
    rank_r = jnp.sum(jnp.where(rowi < coli, same, 0.0), axis=0, keepdims=True)
    count = cnt_ref[...]
    me_f = me.astype(f32)

    def slot_of(owner, rank, index):
        offset = owner - me_f
        offset = jnp.where(offset < 0.0, offset + width, offset)
        return jnp.where(index < count, offset * room + rank, -1.0)

    slot_c = slot_of(own_c, rank_c, iota((slots, 1), 0))
    slot_r = slot_of(own_r[0:1, :], rank_r, iota((1, slots), 1))
    chosen = iota((total, slots), 0).astype(f32) == slot_r
    ids = jnp.sum(jnp.where(chosen, blk_ref[...].astype(f32), 0.0), axis=1, keepdims=True)
    id_hi = jnp.floor(ids * (1.0 / 128.0))
    id_lo = ids - 128.0 * id_hi
    tail = jnp.where(iota((total, 128), 1) < 64, id_lo, id_hi)
    id_out[...] = tail.reshape(width, room, 128).astype(bf16)

    gets[3].wait()
    line8 = iota((group, pts), 0)
    for g in range(groups):
        for c in range(comps):
            rows_f = force_ref[c, g * group:(g + 1) * group, :].astype(f32)
            for i in range(group):
                left_ref[g, c * group:(c + 1) * group, i * pts:(i + 1) * pts] = jnp.where(
                    line8 == i, rows_f, 0.0).astype(bf16)
    gets[4].wait()
    for c in range(comps):
        zs[0, c] = v[c, 0].astype(bf16)
        zs[1, c] = v[c, planes - 1].astype(bf16)

    def halo(src, dst, sem, axis, target):
        return pltpu.make_async_remote_copy(
            src_ref=src, dst_ref=dst, send_sem=h_send.at[sem], recv_sem=h_recv.at[sem],
            device_id={axis: target}, device_id_type=MESH)

    z_down = halo(zs.at[0], zr.at[1], 1, "gz", gz - 1)
    z_up = halo(zs.at[1], zr.at[0], 0, "gz", gz + 1)
    y_down = halo(ys.at[0], yr.at[1], 3, "gy", me - 1)
    y_up = halo(ys.at[1], yr.at[0], 2, "gy", me + 1)

    def enter():
        pl.semaphore_wait(barrier, width - 1 + z_lo.astype(jnp.int32) + z_hi.astype(jnp.int32))
        for there, copy in ((z_lo, z_down), (z_hi, z_up)):
            pl.when(there)(copy.start)

    pl.when(me >= width // 2)(enter)
    for c in range(comps):
        for side, y in ((0, 0), (1, rows - 1)):
            ys[side, c] = jnp.concatenate([v[c, z, y:y + 1, :] for z in range(planes)], axis=0).astype(bf16)
    parts = []
    for pair in range(0, groups, 2):
        both = range(pair, min(pair + 2, groups))
        for g in both:
            get_kern[g].wait()
        for g in both:
            parts.append(jnp.dot(left_ref[g], kv[g * span:(g + 1) * span, :], preferred_element_type=f32))
    spread = jnp.concatenate([
        jnp.concatenate([part[c * group:(c + 1) * group] for part in parts], axis=0)
        for c in range(comps)], axis=1).astype(bf16)
    placed = jnp.dot(jnp.where(chosen, 1.0, 0.0).astype(bf16), spread, preferred_element_type=f32)
    send[...] = placed.reshape(width, room, body).astype(bf16)

    pl.when(me < width // 2)(enter)

    after = width - 1 - me
    right = (after >= me).astype(jnp.int32)
    big = right * after + (1 - right) * me
    small = width - 1 - big
    others = range(1, width)
    far_first = []
    for j in range(width - 1):
        one = (j < big - small).astype(jnp.int32)
        rest = (1 - one) * (j - big + small)
        step = one * (big - j) + (1 - one) * (small - rest // 2)
        far_first.append(me + (2 * right - 1) * (1 - 2 * (rest % 2)) * step)

    def out(src, dst, send_sem, recv_sem, back_by=False):
        def copy(k, target):
            return pltpu.make_async_remote_copy(
                src_ref=src.at[k], dst_ref=dst.at[k], send_sem=send_sem.at[k], recv_sem=recv_sem.at[k],
                device_id={"gy": target}, device_id_type=MESH)

        for target in far_first:
            gap = me - target if back_by else target - me
            copy(lax.rem(gap + width, width), target).start()
        return {k: copy(k, lax.rem(me + k, width)) for k in others}

    tell = out(id_out, id_in, id_send, id_recv)
    go = out(send, recv, go_send, go_recv)
    for there, copy in ((y_lo, y_down), (y_hi, y_up)):
        pl.when(there)(copy.start)
    id_in[0] = id_out[0]
    recv[0] = send[0]

    lane = iota((rows, xcells), 1)
    line = iota((rows, xcells), 0)
    first_x, last_x = lane == 0, lane == xcells - 1
    first_y, last_y = line == 0, line == rows - 1

    def plane(z, carry):
        vx, vy, vz = v[0, z], v[1, z], v[2, z]
        xu_w = jnp.where(last_x, 0.0, coef - half * vx)
        xd_w = jnp.where(first_x, 0.0, coef + half * vx)
        yu_w = jnp.where(last_y, 0.0, coef - half * vy)
        yd_w = jnp.where(first_y, 0.0, coef + half * vy)
        zu_w = jnp.where(z == planes - 1, 0.0, coef - half * vz)
        zd_w = jnp.where(z == 0, 0.0, coef + half * vz)
        above, below = jnp.minimum(z + 1, planes - 1), jnp.maximum(z - 1, 0)
        for c in range(comps):
            mid = v[c, z]
            value = (1.0 - 6.0 * coef) * mid
            value += xu_w * pltpu.roll(mid, xcells - 1, 1) + xd_w * pltpu.roll(mid, 1, 1)
            value += yu_w * pltpu.roll(mid, rows - 1, 0) + yd_w * pltpu.roll(mid, 1, 0)
            value += zu_w * v[c, above] + zd_w * v[c, below]
            fresh[c, z] = value
        return carry

    lax.fori_loop(0, planes, plane, 0)

    for there, copy, buf, z, sign in ((z_lo, z_up, 0, 0, half), (z_hi, z_down, 1, planes - 1, -half)):
        @pl.when(there)
        def _(copy=copy, buf=buf, z=z, sign=sign):
            copy.wait_recv()
            w = coef + sign * v[2, z]
            for c in range(comps):
                fresh[c, z] += w * zr[buf, c].astype(f32)

    for there, copy, buf, y, sign in ((y_lo, y_up, 0, 0, half), (y_hi, y_down, 1, rows - 1, -half)):
        @pl.when(there)
        def _(copy=copy, buf=buf, y=y, sign=sign):
            copy.wait_recv()
            for c in range(comps):
                got = yr[buf, c].astype(f32)
                for z in range(planes):
                    w = coef + sign * v[1, z, y:y + 1, :]
                    fresh[c, z, y:y + 1, :] += w * got[z:z + 1, :]

    for k in others:
        tell[k].wait()
    gid = id_in[...].astype(f32).reshape(total, 128)
    gid = 128.0 * gid[:, 64:65] + gid[:, 0:1]
    ids_r = jnp.sum(jnp.where(iota((total, total), 0) == iota((total, total), 1), gid, 0.0), axis=0, keepdims=True)
    place_r = (iota((zy, total), 0) * nx).astype(f32)
    place_c = (iota((total, zy), 1) * nx).astype(f32)
    puts = [jnp.where(place_r + float(b) == ids_r, time_step, 0.0).astype(bf16) for b in range(nx)]
    takes = [jnp.where(place_c + float(b) == gid, 1.0, 0.0).astype(bf16) for b in range(nx)]
    for k in others:
        go[k].wait()
    got = recv[...].astype(f32).reshape(total, body).astype(bf16)
    for b in range(nx):
        part = jnp.dot(puts[b], got, preferred_element_type=f32)
        for c in range(comps):
            where = (c, slice(None), slice(None), slice(b * cells, (b + 1) * cells))
            value = fresh[where] + part[:, c * cells:(c + 1) * cells].reshape(planes, rows, cells)
            fresh[where] = value
            cells16[c, :, b * cells:(b + 1) * cells] = value.reshape(zy, cells).astype(bf16)
    for c in range(comps):
        part = jnp.zeros((total, cells), f32)
        for b in range(nx):
            part += jnp.dot(takes[b], cells16[c, :, b * cells:(b + 1) * cells], preferred_element_type=f32)
        back[:, :, c * cells:(c + 1) * cells] = part.reshape(width, room, cells).astype(bf16)

    home = out(back, mine, re_send, re_recv, True)
    mine[0] = back[0]

    for there, copy in ((z_lo, z_down), (z_hi, z_up), (y_lo, y_down), (y_hi, y_up)):
        pl.when(there)(copy.wait_send)
    pick = jnp.where(iota((slots, total), 1).astype(f32) == slot_c, 1.0, 0.0).astype(bf16)
    for k in others:
        home[k].wait()
    held = mine[...].astype(f32).reshape(total, body).astype(bf16)
    held_ref[...] = jnp.dot(pick, held, preferred_element_type=f32).astype(bf16)


def sample_kernel(fresh, kv, held_ref, fresh_hbm, out_ref, out_sem):
    comps, slots, pts = out_ref.shape
    cells = kv.shape[1]
    group = 8
    put_v = pltpu.make_async_copy(fresh, fresh_hbm, out_sem)
    put_v.start()
    line8 = iota((group, pts), 0)
    for g in range(slots // group):
        part = held_ref[g * group:(g + 1) * group, :].astype(f32)
        left = jnp.concatenate([part[:, c * cells:(c + 1) * cells] for c in range(comps)], axis=0).astype(bf16)
        result = lax.dot_general(left, kv[g * group * pts:(g + 1) * group * pts, :],
                                 (((1,), (1,)), ((), ())), preferred_element_type=f32)
        for c in range(comps):
            value = jnp.zeros((group, pts), f32)
            for i in range(group):
                value = jnp.where(line8 == i, result[c * group:(c + 1) * group, i * pts:(i + 1) * pts], value)
            out_ref[c, g * group:(g + 1) * group, :] = value
    put_v.wait()


def local(velocity, forces, kernels, owners, blocks, counts):
    width, depth = lax.axis_size("gy"), lax.axis_size("gz")
    slots, comps, pts = forces.shape
    cells = kernels.shape[2]
    _, planes, rows, xcells = velocity.shape
    room = max(2, (2 * slots + width - 1) // width)
    room = (room + 7) // 8 * 8
    total, body = width * room, comps * cells
    vmem = pl.BlockSpec(memory_space=pltpu.VMEM)
    anyw = pl.BlockSpec(memory_space=pltpu.HBM)
    dma = pltpu.SemaphoreType.DMA
    each = dma((width,))
    kept = 4 * velocity.size + 2 * kernels.size + 2 * slots * body
    fresh, kv, held = pl.pallas_call(
        functools.partial(step_kernel, width, depth, room),
        out_shape=(
            pltpu.VMEM(velocity.shape, f32),
            pltpu.VMEM((slots * pts, cells), bf16),
            pltpu.VMEM((slots, body), bf16),
        ),
        in_specs=[anyw] * 6,
        out_specs=(vmem, vmem, vmem),
        scratch_shapes=[
            pltpu.VMEM(velocity.shape, f32),
            pltpu.VMEM((comps, slots, pts), bf16),
            pltpu.VMEM((1, slots), jnp.int32),
            pltpu.VMEM((1, slots), jnp.int32),
            pltpu.VMEM((1, 1), jnp.int32),
            pltpu.VMEM((comps, planes * rows, xcells), bf16),
            pltpu.VMEM((slots // 8, comps * 8, 8 * pts), bf16),
            pltpu.VMEM((width, room, 128), bf16),
            pltpu.VMEM((width, room, 128), bf16),
            pltpu.VMEM((width, room, body), bf16),
            pltpu.VMEM((width, room, body), bf16),
            pltpu.VMEM((width, room, body), bf16),
            pltpu.VMEM((width, room, body), bf16),
            pltpu.VMEM((2, comps, rows, xcells), bf16),
            pltpu.VMEM((2, comps, rows, xcells), bf16),
            pltpu.VMEM((2, comps, planes, xcells), bf16),
            pltpu.VMEM((2, comps, planes, xcells), bf16),
            dma((5,)), dma((slots // 8,)), each, each, each, each, each, each, dma((4,)), dma((4,)),
        ],
        compiler_params=pltpu.CompilerParams(
            collective_id=0, has_side_effects=True, vmem_limit_bytes=vmem_bytes - kept - 512 * 1024),
        name="boundary_step",
    )(velocity, forces.transpose(1, 0, 2), kernels.reshape(slots * pts, cells),
      owners.reshape(1, slots), blocks.reshape(1, slots), counts.reshape(1, 1))
    fresh, sampled = pl.pallas_call(
        sample_kernel,
        out_shape=(
            jax.ShapeDtypeStruct(velocity.shape, f32),
            jax.ShapeDtypeStruct((comps, slots, pts), f32),
        ),
        in_specs=[vmem, vmem, vmem],
        out_specs=(anyw, vmem),
        scratch_shapes=[dma],
        compiler_params=pltpu.CompilerParams(vmem_limit_bytes=24 * 2**20),
        name="sample_points",
    )(fresh, kv, held)
    return fresh, sampled.transpose(1, 0, 2)


def solution(mesh):
    return jax.shard_map(
        local,
        mesh=mesh,
        in_specs=(
            P(None, "gz", "gy", None),
            P(("gz", "gy"), None, None),
            P(("gz", "gy"), None, None),
            P(("gz", "gy"), None),
            P(("gz", "gy")),
            P(("gz", "gy")),
        ),
        out_specs=(P(None, "gz", "gy", None), P(("gz", "gy"), None, None)),
        check_vma=False,
    )
```

```python
import functools

import jax
import jax.numpy as jnp
from jax import lax
from jax.experimental import pallas as pl
from jax.experimental.pallas import tpu as pltpu
from jax.sharding import PartitionSpec as P

time_step = 0.25
vmem_bytes = 67043328
viscosity = 0.5
MESH = pl.DeviceIdType.MESH
f32 = jnp.float32
bf16 = jnp.bfloat16


def iota(shape, dim):
    return lax.broadcasted_iota(jnp.int32, shape, dim)


def step_kernel(width, depth, room, vel_hbm, force_hbm, kern_hbm, own_hbm, blk_hbm, cnt_hbm,
                fresh, kvt, held_ref,
                v, kv, force_ref, own_ref, blk_ref, cnt_ref, cells16, left_ref, id_out, id_in, send, recv, back, mine,
                zs, zr, ys, yr,
                in_sem, kern_sem, id_sems, go_sems, re_sems, h_send, h_recv):
    me = lax.axis_index("gy")
    gz = lax.axis_index("gz")
    comps, planes, rows, xcells = v.shape
    _, slots, pts = force_ref.shape
    cells = kv.shape[1]
    nx = xcells // cells
    zy = planes * rows
    total = width * room
    body = comps * cells
    coef = time_step * viscosity
    half = time_step * 0.5
    group = 8
    groups = slots // group
    span = group * pts

    barrier = pltpu.get_barrier_semaphore()
    for k in range(1, width):
        pl.semaphore_signal(barrier, inc=1, device_id={"gy": lax.rem(me + k, width)}, device_id_type=MESH)
    z_lo, z_hi = gz > 0, gz < depth - 1
    y_lo, y_hi = me > 0, me < width - 1

    @pl.when(z_lo)
    def _():
        pl.semaphore_signal(barrier, inc=1, device_id={"gz": gz - 1}, device_id_type=MESH)

    @pl.when(z_hi)
    def _():
        pl.semaphore_signal(barrier, inc=1, device_id={"gz": gz + 1}, device_id_type=MESH)

    inner = pl.ds(1, planes - 2)
    gets = [pltpu.make_async_copy(src, dst, in_sem.at[i]) for i, (src, dst) in enumerate((
        (own_hbm, own_ref), (blk_hbm, blk_ref), (cnt_hbm, cnt_ref), (force_hbm, force_ref),
        (vel_hbm.at[:, 0], v.at[:, 0]), (vel_hbm.at[:, planes - 1], v.at[:, planes - 1]),
        (vel_hbm.at[:, inner], v.at[:, inner])))]
    halves = 2 if groups % 2 == 0 else 1
    part_rows = groups // halves * span
    get_kern = [pltpu.make_async_copy(kern_hbm.at[pl.ds(h * part_rows, part_rows)],
                                      kv.at[pl.ds(h * part_rows, part_rows)], kern_sem.at[h])
                for h in range(halves)]
    for copy in gets[:6] + get_kern + gets[6:]:
        copy.start()

    for copy in gets[:3]:
        copy.wait()
    rowi, coli = iota((slots, slots), 0), iota((slots, slots), 1)
    own_r = jnp.broadcast_to(own_ref[...].astype(f32), (slots, slots))
    own_c = jnp.sum(jnp.where(rowi == coli, own_r, 0.0), axis=1, keepdims=True)
    same = jnp.where(own_r == own_c, 1.0, 0.0)
    rank_c = jnp.sum(jnp.where(coli < rowi, same, 0.0), axis=1, keepdims=True)
    rank_r = jnp.sum(jnp.where(rowi < coli, same, 0.0), axis=0, keepdims=True)
    count = cnt_ref[...]
    me_f = me.astype(f32)

    def slot_of(owner, rank, index):
        offset = owner - me_f
        offset = jnp.where(offset < 0.0, offset + width, offset)
        return jnp.where(index < count, offset * room + rank, -1.0)

    slot_c = slot_of(own_c, rank_c, iota((slots, 1), 0))
    slot_r = slot_of(own_r[0:1, :], rank_r, iota((1, slots), 1))
    chosen = iota((total, slots), 0).astype(f32) == slot_r
    ids = jnp.sum(jnp.where(chosen, blk_ref[...].astype(f32), 0.0), axis=1, keepdims=True)
    id_hi = jnp.floor(ids * (1.0 / 128.0))
    id_lo = ids - 128.0 * id_hi
    tail = jnp.where(iota((total, 128), 1) < 64, id_lo, id_hi)
    id_out[...] = tail.reshape(width, room, 128).astype(bf16)

    gets[3].wait()
    line8 = iota((group, pts), 0)
    for g in range(groups):
        for c in range(comps):
            rows_f = force_ref[c, g * group:(g + 1) * group, :].astype(f32)
            for i in range(group):
                left_ref[g, c * group:(c + 1) * group, i * pts:(i + 1) * pts] = jnp.where(
                    line8 == i, rows_f, 0.0).astype(bf16)
    gets[4].wait()
    gets[5].wait()
    for c in range(comps):
        zs[0, c] = v[c, 0].astype(bf16)
        zs[1, c] = v[c, planes - 1].astype(bf16)

    def halo(src, dst, sem, axis, target):
        return pltpu.make_async_remote_copy(
            src_ref=src, dst_ref=dst, send_sem=h_send.at[sem], recv_sem=h_recv.at[sem],
            device_id={axis: target}, device_id_type=MESH)

    z_down = halo(zs.at[0], zr.at[1], 1, "gz", gz - 1)
    z_up = halo(zs.at[1], zr.at[0], 0, "gz", gz + 1)
    y_down = halo(ys.at[0], yr.at[1], 3, "gy", me - 1)
    y_up = halo(ys.at[1], yr.at[0], 2, "gy", me + 1)

    def enter():
        pl.semaphore_wait(barrier, width - 1 + z_lo.astype(jnp.int32) + z_hi.astype(jnp.int32))
        for there, copy in ((z_lo, z_down), (z_hi, z_up)):
            pl.when(there)(copy.start)

    pl.when(me >= width // 2)(enter)
    parts = []
    for h in range(halves):
        get_kern[h].wait()
        for g in range(h * groups // halves, (h + 1) * groups // halves):
            parts.append(jnp.dot(left_ref[g], kv[g * span:(g + 1) * span, :], preferred_element_type=f32))
    spread = jnp.concatenate([
        jnp.concatenate([part[c * group:(c + 1) * group] for part in parts], axis=0)
        for c in range(comps)], axis=1).astype(bf16)
    placed = jnp.dot(jnp.where(chosen, 1.0, 0.0).astype(bf16), spread, preferred_element_type=f32)
    send[...] = placed.reshape(width, room, body).astype(bf16)

    gets[6].wait()
    for c in range(comps):
        for side, y in ((0, 0), (1, rows - 1)):
            ys[side, c] = jnp.concatenate([v[c, z, y:y + 1, :] for z in range(planes)], axis=0).astype(bf16)
    pl.when(me < width // 2)(enter)

    after = width - 1 - me
    right = (after >= me).astype(jnp.int32)
    big = right * after + (1 - right) * me
    small = width - 1 - big
    far_first = []
    for j in range(width - 1):
        one = (j < big - small).astype(jnp.int32)
        rest = (1 - one) * (j - big + small)
        step = one * (big - j) + (1 - one) * (small - rest // 2)
        far_first.append(me + (2 * right - 1) * (1 - 2 * (rest % 2)) * step)

    def out(src, dst, sems, back_by=False):
        for target in far_first:
            gap = me - target if back_by else target - me
            k = lax.rem(gap + width, width)
            pltpu.make_async_remote_copy(
                src_ref=src.at[k], dst_ref=dst.at[k], send_sem=sems.at[0], recv_sem=sems.at[1],
                device_id={"gy": target}, device_id_type=MESH).start()
        rest = pl.ds(1, width - 1)
        return pltpu.make_async_remote_copy(
            src_ref=src.at[rest], dst_ref=dst.at[rest], send_sem=sems.at[0], recv_sem=sems.at[1],
            device_id={"gy": far_first[0]}, device_id_type=MESH)

    tell = out(id_out, id_in, id_sems)
    go = out(send, recv, go_sems)
    for there, copy in ((y_lo, y_down), (y_hi, y_up)):
        pl.when(there)(copy.start)
    id_in[0] = id_out[0]
    recv[0] = send[0]

    lane = iota((rows, xcells), 1)
    line = iota((rows, xcells), 0)
    first_x, last_x = lane == 0, lane == xcells - 1
    first_y, last_y = line == 0, line == rows - 1

    def plane(z, carry):
        vx, vy, vz = v[0, z], v[1, z], v[2, z]
        xu_w = jnp.where(last_x, 0.0, coef - half * vx)
        xd_w = jnp.where(first_x, 0.0, coef + half * vx)
        yu_w = jnp.where(last_y, 0.0, coef - half * vy)
        yd_w = jnp.where(first_y, 0.0, coef + half * vy)
        zu_w = jnp.where(z == planes - 1, 0.0, coef - half * vz)
        zd_w = jnp.where(z == 0, 0.0, coef + half * vz)
        above, below = jnp.minimum(z + 1, planes - 1), jnp.maximum(z - 1, 0)
        for c in range(comps):
            mid = v[c, z]
            value = (1.0 - 6.0 * coef) * mid
            value += xu_w * pltpu.roll(mid, xcells - 1, 1) + xd_w * pltpu.roll(mid, 1, 1)
            value += yu_w * pltpu.roll(mid, rows - 1, 0) + yd_w * pltpu.roll(mid, 1, 0)
            value += zu_w * v[c, above] + zd_w * v[c, below]
            fresh[c, z] = value
        return carry

    lax.fori_loop(0, planes, plane, 0)

    for there, copy, buf, z, sign in ((z_lo, z_up, 0, 0, half), (z_hi, z_down, 1, planes - 1, -half)):
        @pl.when(there)
        def _(copy=copy, buf=buf, z=z, sign=sign):
            copy.wait_recv()
            w = coef + sign * v[2, z]
            for c in range(comps):
                fresh[c, z] += w * zr[buf, c].astype(f32)

    for there, copy, buf, y, sign in ((y_lo, y_up, 0, 0, half), (y_hi, y_down, 1, rows - 1, -half)):
        @pl.when(there)
        def _(copy=copy, buf=buf, y=y, sign=sign):
            copy.wait_recv()
            for c in range(comps):
                got = yr[buf, c].astype(f32)
                for z in range(planes):
                    w = coef + sign * v[1, z, y:y + 1, :]
                    fresh[c, z, y:y + 1, :] += w * got[z:z + 1, :]

    tell.wait()
    gid = id_in[...].astype(f32).reshape(total, 128)
    gid = 128.0 * gid[:, 64:65] + gid[:, 0:1]
    ids_r = jnp.sum(jnp.where(iota((total, total), 0) == iota((total, total), 1), gid, 0.0), axis=0, keepdims=True)
    place_r = (iota((zy, total), 0) * nx).astype(f32)
    place_c = (iota((total, zy), 1) * nx).astype(f32)
    puts = [jnp.where(place_r + float(b) == ids_r, time_step, 0.0).astype(bf16) for b in range(nx)]
    takes = [jnp.where(place_c + float(b) == gid, 1.0, 0.0).astype(bf16) for b in range(nx)]
    go.wait()
    got = recv[...].astype(f32).reshape(total, body).astype(bf16)
    for b in range(nx):
        part = jnp.dot(puts[b], got, preferred_element_type=f32)
        for c in range(comps):
            where = (c, slice(None), slice(None), slice(b * cells, (b + 1) * cells))
            value = fresh[where] + part[:, c * cells:(c + 1) * cells].reshape(planes, rows, cells)
            fresh[where] = value
            cells16[c, :, b * cells:(b + 1) * cells] = value.reshape(zy, cells).astype(bf16)
    for c in range(comps):
        part = jnp.zeros((total, cells), f32)
        for b in range(nx):
            part += jnp.dot(takes[b], cells16[c, :, b * cells:(b + 1) * cells], preferred_element_type=f32)
        back[:, :, c * cells:(c + 1) * cells] = part.reshape(width, room, cells).astype(bf16)

    home = out(back, mine, re_sems, True)
    mine[0] = back[0]

    for t in range(slots * pts // cells):
        kvt[:, t * cells:(t + 1) * cells] = kv[t * cells:(t + 1) * cells, :].T
    for there, copy in ((z_lo, z_down), (z_hi, z_up), (y_lo, y_down), (y_hi, y_up)):
        pl.when(there)(copy.wait_send)
    pick = jnp.where(iota((slots, total), 1).astype(f32) == slot_c, 1.0, 0.0).astype(bf16)
    home.wait()
    held = mine[...].astype(f32).reshape(total, body).astype(bf16)
    held_ref[...] = jnp.dot(pick, held, preferred_element_type=f32).astype(bf16)


def sample_kernel(fresh, kvt, held_ref, fresh_hbm, out_hbm, out_ref, out_sem):
    comps, slots, pts = out_ref.shape
    cells = kvt.shape[0]
    group = 8
    put_v = pltpu.make_async_copy(fresh, fresh_hbm, out_sem.at[0])
    put_v.start()
    line8 = iota((group, pts), 0)
    for g in range(slots // group):
        part = held_ref[g * group:(g + 1) * group, :].astype(f32)
        left = jnp.concatenate([part[:, c * cells:(c + 1) * cells] for c in range(comps)], axis=0).astype(bf16)
        result = jnp.dot(left, kvt[:, g * group * pts:(g + 1) * group * pts], preferred_element_type=f32)
        for c in range(comps):
            value = jnp.zeros((group, pts), f32)
            for i in range(group):
                value = jnp.where(line8 == i, result[c * group:(c + 1) * group, i * pts:(i + 1) * pts], value)
            out_ref[c, g * group:(g + 1) * group, :] = value
    put_p = pltpu.make_async_copy(out_ref, out_hbm, out_sem.at[1])
    put_p.start()
    put_v.wait()
    put_p.wait()


def local(velocity, forces, kernels, owners, blocks, counts):
    width, depth = lax.axis_size("gy"), lax.axis_size("gz")
    slots, comps, pts = forces.shape
    cells = kernels.shape[2]
    _, planes, rows, xcells = velocity.shape
    room = max(2, (2 * slots + width - 1) // width)
    room = (room + 7) // 8 * 8
    total, body = width * room, comps * cells
    vmem = pl.BlockSpec(memory_space=pltpu.VMEM)
    anyw = pl.BlockSpec(memory_space=pltpu.HBM)
    dma = pltpu.SemaphoreType.DMA
    pair = dma((2,))
    kept = 4 * velocity.size + 2 * kernels.size + 2 * slots * body
    fresh, kvt, held = pl.pallas_call(
        functools.partial(step_kernel, width, depth, room),
        out_shape=(
            pltpu.VMEM(velocity.shape, f32),
            pltpu.VMEM((cells, slots * pts), bf16),
            pltpu.VMEM((slots, body), bf16),
        ),
        in_specs=[anyw] * 6,
        out_specs=(vmem, vmem, vmem),
        scratch_shapes=[
            pltpu.VMEM(velocity.shape, f32),
            pltpu.VMEM((slots * pts, cells), bf16),
            pltpu.VMEM((comps, slots, pts), bf16),
            pltpu.VMEM((1, slots), jnp.int32),
            pltpu.VMEM((1, slots), jnp.int32),
            pltpu.VMEM((1, 1), jnp.int32),
            pltpu.VMEM((comps, planes * rows, xcells), bf16),
            pltpu.VMEM((slots // 8, comps * 8, 8 * pts), bf16),
            pltpu.VMEM((width, room, 128), bf16),
            pltpu.VMEM((width, room, 128), bf16),
            pltpu.VMEM((width, room, body), bf16),
            pltpu.VMEM((width, room, body), bf16),
            pltpu.VMEM((width, room, body), bf16),
            pltpu.VMEM((width, room, body), bf16),
            pltpu.VMEM((2, comps, rows, xcells), bf16),
            pltpu.VMEM((2, comps, rows, xcells), bf16),
            pltpu.VMEM((2, comps, planes, xcells), bf16),
            pltpu.VMEM((2, comps, planes, xcells), bf16),
            dma((7,)), dma((2,)), pair, pair, pair, dma((4,)), dma((4,)),
        ],
        compiler_params=pltpu.CompilerParams(
            collective_id=0, has_side_effects=True, vmem_limit_bytes=vmem_bytes - kept - 512 * 1024),
        name="boundary_step",
    )(velocity, forces.transpose(1, 0, 2), kernels.reshape(slots * pts, cells),
      owners.reshape(1, slots), blocks.reshape(1, slots), counts.reshape(1, 1))
    fresh, sampled = pl.pallas_call(
        sample_kernel,
        out_shape=(
            jax.ShapeDtypeStruct(velocity.shape, f32),
            jax.ShapeDtypeStruct((comps, slots, pts), f32),
        ),
        in_specs=[vmem, vmem, vmem],
        out_specs=(anyw, anyw),
        scratch_shapes=[pltpu.VMEM((comps, slots, pts), f32), dma((2,))],
        compiler_params=pltpu.CompilerParams(vmem_limit_bytes=24 * 2**20),
        name="sample_points",
    )(fresh, kvt, held)
    return fresh, sampled.transpose(1, 0, 2)


def solution(mesh):
    return jax.shard_map(
        local,
        mesh=mesh,
        in_specs=(
            P(None, "gz", "gy", None),
            P(("gz", "gy"), None, None),
            P(("gz", "gy"), None, None),
            P(("gz", "gy"), None),
            P(("gz", "gy")),
            P(("gz", "gy")),
        ),
        out_specs=(P(None, "gz", "gy", None), P(("gz", "gy"), None, None)),
        check_vma=False,
    )
```

```python
import functools

import jax
import jax.numpy as jnp
from jax import lax
from jax.experimental import pallas as pl
from jax.experimental.pallas import tpu as pltpu
from jax.sharding import PartitionSpec as P

time_step = 0.25
vmem_bytes = 67043328
viscosity = 0.5
MESH = pl.DeviceIdType.MESH
f32 = jnp.float32
bf16 = jnp.bfloat16


def iota(shape, dim):
    return lax.broadcasted_iota(jnp.int32, shape, dim)


def step_kernel(width, depth, room, vel_hbm, force_hbm, kern_hbm, own_hbm, blk_hbm, cnt_hbm,
                fresh, kvt, held_ref,
                v, kv, force_ref, own_ref, blk_ref, cnt_ref, cells16, edge, pre, left_ref, id_out, id_in, send, recv, back, mine,
                zs, zr, ys, yr,
                in_sem, kern_sem, id_sems, go_sems, re_sems, h_send, h_recv):
    me = lax.axis_index("gy")
    gz = lax.axis_index("gz")
    comps, planes, rows, xcells = v.shape
    _, slots, pts = force_ref.shape
    cells = kv.shape[1]
    nx = xcells // cells
    zy = planes * rows
    total = width * room
    body = comps * cells
    coef = time_step * viscosity
    half = time_step * 0.5
    group = 8
    groups = slots // group
    span = group * pts

    barrier = pltpu.get_barrier_semaphore()
    for k in range(1, width):
        pl.semaphore_signal(barrier, inc=1, device_id={"gy": lax.rem(me + k, width)}, device_id_type=MESH)
    z_lo, z_hi = gz > 0, gz < depth - 1
    y_lo, y_hi = me > 0, me < width - 1

    @pl.when(z_lo)
    def _():
        pl.semaphore_signal(barrier, inc=1, device_id={"gz": gz - 1}, device_id_type=MESH)

    @pl.when(z_hi)
    def _():
        pl.semaphore_signal(barrier, inc=1, device_id={"gz": gz + 1}, device_id_type=MESH)

    inner = pl.ds(1, planes - 2)
    gets = [pltpu.make_async_copy(src, dst, in_sem.at[i]) for i, (src, dst) in enumerate((
        (own_hbm, own_ref), (blk_hbm, blk_ref), (cnt_hbm, cnt_ref), (force_hbm, force_ref),
        (vel_hbm.at[:, 0], v.at[:, 0]), (vel_hbm.at[:, planes - 1], v.at[:, planes - 1]),
        (vel_hbm.at[:, :, 0], edge.at[0]), (vel_hbm.at[:, :, rows - 1], edge.at[1]),
        (vel_hbm.at[:, inner], v.at[:, inner])))]
    halves = 2 if groups % 2 == 0 else 1
    part_rows = groups // halves * span
    get_kern = [pltpu.make_async_copy(kern_hbm.at[pl.ds(h * part_rows, part_rows)],
                                      kv.at[pl.ds(h * part_rows, part_rows)], kern_sem.at[h])
                for h in range(halves)]
    for copy in gets[:8] + get_kern + gets[8:]:
        copy.start()

    for copy in gets[:3]:
        copy.wait()
    rowi, coli = iota((slots, slots), 0), iota((slots, slots), 1)
    own_r = jnp.broadcast_to(own_ref[...].astype(f32), (slots, slots))
    own_c = jnp.sum(jnp.where(rowi == coli, own_r, 0.0), axis=1, keepdims=True)
    same = jnp.where(own_r == own_c, 1.0, 0.0)
    rank_c = jnp.sum(jnp.where(coli < rowi, same, 0.0), axis=1, keepdims=True)
    rank_r = jnp.sum(jnp.where(rowi < coli, same, 0.0), axis=0, keepdims=True)
    count = cnt_ref[...]
    me_f = me.astype(f32)

    def slot_of(owner, rank, index):
        offset = owner - me_f
        offset = jnp.where(offset < 0.0, offset + width, offset)
        return jnp.where(index < count, offset * room + rank, -1.0)

    slot_c = slot_of(own_c, rank_c, iota((slots, 1), 0))
    slot_r = slot_of(own_r[0:1, :], rank_r, iota((1, slots), 1))
    chosen = iota((total, slots), 0).astype(f32) == slot_r
    ids = jnp.sum(jnp.where(chosen, blk_ref[...].astype(f32) + 1.0, 0.0), axis=1, keepdims=True) - 1.0
    slot_lane = iota((room, 128), 1) == iota((room, 128), 0)
    for k in range(width):
        id_out[k] = jnp.sum(jnp.where(slot_lane, ids[k * room:(k + 1) * room], 0.0), axis=0, keepdims=True)

    gets[3].wait()
    line8 = iota((group, pts), 0)
    for g in range(groups):
        for c in range(comps):
            rows_f = force_ref[c, g * group:(g + 1) * group, :].astype(f32)
            for i in range(group):
                left_ref[g, c * group:(c + 1) * group, i * pts:(i + 1) * pts] = jnp.where(
                    line8 == i, rows_f, 0.0).astype(bf16)
    gets[4].wait()
    gets[5].wait()
    for c in range(comps):
        zs[0, c] = v[c, 0].astype(bf16)
        zs[1, c] = v[c, planes - 1].astype(bf16)

    def halo(src, dst, sem, axis, target):
        return pltpu.make_async_remote_copy(
            src_ref=src, dst_ref=dst, send_sem=h_send.at[sem], recv_sem=h_recv.at[sem],
            device_id={axis: target}, device_id_type=MESH)

    z_down = halo(zs.at[0], zr.at[1], 1, "gz", gz - 1)
    z_up = halo(zs.at[1], zr.at[0], 0, "gz", gz + 1)
    y_down = halo(ys.at[0], yr.at[1], 3, "gy", me - 1)
    y_up = halo(ys.at[1], yr.at[0], 2, "gy", me + 1)

    early = me >= width // 2
    late = jnp.logical_not(early)

    def enter():
        pl.semaphore_wait(barrier, width - 1 + z_lo.astype(jnp.int32) + z_hi.astype(jnp.int32))

    def start_z(when):
        for there, copy in ((z_lo, z_down), (z_hi, z_up)):
            pl.when(jnp.logical_and(when, there))(copy.start)

    def start_y(when):
        for there, copy in ((y_lo, y_down), (y_hi, y_up)):
            pl.when(jnp.logical_and(when, there))(copy.start)

    pl.when(early)(enter)
    start_z(early)
    gets[6].wait()
    gets[7].wait()
    ys[...] = edge[...].astype(bf16)
    start_y(early)
    parts = []
    for h in range(halves):
        get_kern[h].wait()
        for g in range(h * groups // halves, (h + 1) * groups // halves):
            parts.append(jnp.dot(left_ref[g], kv[g * span:(g + 1) * span, :], preferred_element_type=f32))
    spread = jnp.concatenate([
        jnp.concatenate([part[c * group:(c + 1) * group] for part in parts], axis=0)
        for c in range(comps)], axis=1).astype(bf16)
    placed = jnp.dot(jnp.where(chosen, 1.0, 0.0).astype(bf16), spread, preferred_element_type=f32)
    send[...] = placed.reshape(width, room, body).astype(bf16)

    pl.when(late)(enter)
    start_z(late)

    after = width - 1 - me
    right = (after >= me).astype(jnp.int32)
    big = right * after + (1 - right) * me
    small = width - 1 - big
    far_first = []
    for j in range(width - 1):
        one = (j < big - small).astype(jnp.int32)
        rest = (1 - one) * (j - big + small)
        step = one * (big - j) + (1 - one) * (small - rest // 2)
        far_first.append(me + (2 * right - 1) * (1 - 2 * (rest % 2)) * step)

    def out(src, dst, sems, targets, back_by=False):
        for target in targets:
            gap = me - target if back_by else target - me
            k = lax.rem(gap + width, width)
            pltpu.make_async_remote_copy(
                src_ref=src.at[k], dst_ref=dst.at[k], send_sem=sems.at[0], recv_sem=sems.at[1],
                device_id={"gy": target}, device_id_type=MESH).start()

    def sent(src, dst, sems):
        rest = pl.ds(1, width - 1)
        return pltpu.make_async_remote_copy(
            src_ref=src.at[rest], dst_ref=dst.at[rest], send_sem=sems.at[0], recv_sem=sems.at[1],
            device_id={"gy": far_first[0]}, device_id_type=MESH)

    out(id_out, id_in, id_sems, far_first)
    out(send, recv, go_sems, far_first[:2])
    start_y(late)
    out(send, recv, go_sems, far_first[2:])
    id_in[0] = id_out[0]
    recv[0] = send[0]

    gets[8].wait()
    lane = iota((rows, xcells), 1)
    line = iota((rows, xcells), 0)
    first_x, last_x = lane == 0, lane == xcells - 1
    first_y, last_y = line == 0, line == rows - 1

    def plane(z, carry):
        vx, vy, vz = v[0, z], v[1, z], v[2, z]
        xu_w = jnp.where(last_x, 0.0, coef - half * vx)
        xd_w = jnp.where(first_x, 0.0, coef + half * vx)
        yu_w = jnp.where(last_y, 0.0, coef - half * vy)
        yd_w = jnp.where(first_y, 0.0, coef + half * vy)
        zu_w = jnp.where(z == planes - 1, 0.0, coef - half * vz)
        zd_w = jnp.where(z == 0, 0.0, coef + half * vz)
        above, below = jnp.minimum(z + 1, planes - 1), jnp.maximum(z - 1, 0)
        for c in range(comps):
            mid = v[c, z]
            value = (1.0 - 6.0 * coef) * mid
            value += xu_w * pltpu.roll(mid, xcells - 1, 1) + xd_w * pltpu.roll(mid, 1, 1)
            value += yu_w * pltpu.roll(mid, rows - 1, 0) + yd_w * pltpu.roll(mid, 1, 0)
            value += zu_w * v[c, above] + zd_w * v[c, below]
            fresh[c, z] = value
        return carry

    lax.fori_loop(0, planes, plane, 0)

    for there, copy, buf, y, sign in ((y_lo, y_up, 0, 0, half), (y_hi, y_down, 1, rows - 1, -half)):
        @pl.when(there)
        def _(copy=copy, buf=buf, y=y, sign=sign):
            copy.wait_recv()
            for c in range(comps):
                got = yr[buf, c].astype(f32)
                for z in range(planes):
                    w = coef + sign * v[1, z, y:y + 1, :]
                    fresh[c, z, y:y + 1, :] += w * got[z:z + 1, :]

    sent(id_out, id_in, id_sems).wait()
    theirs = jnp.concatenate([jnp.broadcast_to(id_in[k], (room, 128)) for k in range(width)], axis=0)
    slot_lane = iota((total, 128), 1) == iota((total, 128), 0) % room
    theirs = jnp.sum(jnp.where(slot_lane, theirs, 0.0), axis=1, keepdims=True)
    place = (iota((total, zy), 1) * nx).astype(f32)
    takes = [jnp.where(place + float(b) == theirs, 1.0, 0.0).astype(bf16) for b in range(nx)]
    every = jnp.concatenate(takes, axis=1)
    match = lax.dot_general(every, every, (((1,), (1,)), ((), ())), preferred_element_type=f32)
    match = (match * time_step).astype(bf16)
    for there, copy, buf, z, sign in ((z_lo, z_up, 0, 0, half), (z_hi, z_down, 1, planes - 1, -half)):
        @pl.when(there)
        def _(copy=copy, buf=buf, z=z, sign=sign):
            copy.wait_recv()
            w = coef + sign * v[2, z]
            for c in range(comps):
                fresh[c, z] += w * zr[buf, c].astype(f32)

    def split(z, carry):
        at = pl.ds(pl.multiple_of(z * rows, rows), rows)
        low = pl.ds(pl.multiple_of(zy + z * rows, rows), rows)
        for c in range(comps):
            value = fresh[c, z]
            high = value.astype(bf16)
            cells16[c, at, :] = high
            cells16[c, low, :] = (value - high.astype(f32)).astype(bf16)
        return carry

    lax.fori_loop(0, planes, split, 0)

    twice = [jnp.concatenate([take, take], axis=1) for take in takes]
    for c in range(comps):
        part = jnp.dot(twice[0], cells16[c, :, :cells], preferred_element_type=f32)
        for b in range(1, nx):
            part += jnp.dot(twice[b], cells16[c, :, b * cells:(b + 1) * cells], preferred_element_type=f32)
        pre[:, c * cells:(c + 1) * cells] = part
    sent(send, recv, go_sems).wait()
    got = recv[...].astype(f32).reshape(total, body).astype(bf16)
    force = jnp.dot(match, got, preferred_element_type=f32)
    back[...] = (pre[...] + force).reshape(width, room, body).astype(bf16)

    out(back, mine, re_sems, far_first, True)
    mine[0] = back[0]

    for b in range(nx):
        put = (takes[b].astype(f32) * time_step).T.astype(bf16)
        part = jnp.dot(put, got, preferred_element_type=f32)
        for c in range(comps):
            where = (c, slice(None), slice(None), slice(b * cells, (b + 1) * cells))
            fresh[where] += part[:, c * cells:(c + 1) * cells].reshape(planes, rows, cells)
    for t in range(slots * pts // cells):
        kvt[:, t * cells:(t + 1) * cells] = kv[t * cells:(t + 1) * cells, :].T
    for there, copy in ((z_lo, z_down), (z_hi, z_up), (y_lo, y_down), (y_hi, y_up)):
        pl.when(there)(copy.wait_send)
    pick = jnp.where(iota((slots, total), 1).astype(f32) == slot_c, 1.0, 0.0).astype(bf16)
    sent(back, mine, re_sems).wait()
    held = mine[...].astype(f32).reshape(total, body).astype(bf16)
    held_ref[...] = jnp.dot(pick, held, preferred_element_type=f32).astype(bf16)


def sample_kernel(fresh, kvt, held_ref, fresh_hbm, out_hbm, out_ref, out_sem):
    comps, slots, pts = out_ref.shape
    cells = kvt.shape[0]
    group = 8
    put_v = pltpu.make_async_copy(fresh, fresh_hbm, out_sem.at[0])
    put_v.start()
    line8 = iota((group, pts), 0)
    for g in range(slots // group):
        part = held_ref[g * group:(g + 1) * group, :].astype(f32)
        left = jnp.concatenate([part[:, c * cells:(c + 1) * cells] for c in range(comps)], axis=0).astype(bf16)
        result = jnp.dot(left, kvt[:, g * group * pts:(g + 1) * group * pts], preferred_element_type=f32)
        for c in range(comps):
            value = jnp.zeros((group, pts), f32)
            for i in range(group):
                value = jnp.where(line8 == i, result[c * group:(c + 1) * group, i * pts:(i + 1) * pts], value)
            out_ref[c, g * group:(g + 1) * group, :] = value
    put_p = pltpu.make_async_copy(out_ref, out_hbm, out_sem.at[1])
    put_p.start()
    put_v.wait()
    put_p.wait()


def local(velocity, forces, kernels, owners, blocks, counts):
    width, depth = lax.axis_size("gy"), lax.axis_size("gz")
    slots, comps, pts = forces.shape
    cells = kernels.shape[2]
    _, planes, rows, xcells = velocity.shape
    room = max(2, (2 * slots + width - 1) // width)
    room = (room + 7) // 8 * 8
    total, body = width * room, comps * cells
    vmem = pl.BlockSpec(memory_space=pltpu.VMEM)
    anyw = pl.BlockSpec(memory_space=pltpu.HBM)
    dma = pltpu.SemaphoreType.DMA
    pair = dma((2,))
    kept = 4 * velocity.size + 2 * kernels.size + 2 * slots * body
    fresh, kvt, held = pl.pallas_call(
        functools.partial(step_kernel, width, depth, room),
        out_shape=(
            pltpu.VMEM(velocity.shape, f32),
            pltpu.VMEM((cells, slots * pts), bf16),
            pltpu.VMEM((slots, body), bf16),
        ),
        in_specs=[anyw] * 6,
        out_specs=(vmem, vmem, vmem),
        scratch_shapes=[
            pltpu.VMEM(velocity.shape, f32),
            pltpu.VMEM((slots * pts, cells), bf16),
            pltpu.VMEM((comps, slots, pts), bf16),
            pltpu.VMEM((1, slots), jnp.int32),
            pltpu.VMEM((1, slots), jnp.int32),
            pltpu.VMEM((1, 1), jnp.int32),
            pltpu.VMEM((comps, 2 * planes * rows, xcells), bf16),
            pltpu.VMEM((2, comps, planes, xcells), f32),
            pltpu.VMEM((total, body), f32),
            pltpu.VMEM((slots // 8, comps * 8, 8 * pts), bf16),
            pltpu.VMEM((width, 1, 128), f32),
            pltpu.VMEM((width, 1, 128), f32),
            pltpu.VMEM((width, room, body), bf16),
            pltpu.VMEM((width, room, body), bf16),
            pltpu.VMEM((width, room, body), bf16),
            pltpu.VMEM((width, room, body), bf16),
            pltpu.VMEM((2, comps, rows, xcells), bf16),
            pltpu.VMEM((2, comps, rows, xcells), bf16),
            pltpu.VMEM((2, comps, planes, xcells), bf16),
            pltpu.VMEM((2, comps, planes, xcells), bf16),
            dma((9,)), dma((2,)), pair, pair, pair, dma((4,)), dma((4,)),
        ],
        compiler_params=pltpu.CompilerParams(
            collective_id=0, has_side_effects=True, vmem_limit_bytes=vmem_bytes - kept - 512 * 1024),
        name="boundary_step",
    )(velocity, forces.transpose(1, 0, 2), kernels.reshape(slots * pts, cells),
      owners.reshape(1, slots), blocks.reshape(1, slots), counts.reshape(1, 1))
    fresh, sampled = pl.pallas_call(
        sample_kernel,
        out_shape=(
            jax.ShapeDtypeStruct(velocity.shape, f32),
            jax.ShapeDtypeStruct((comps, slots, pts), f32),
        ),
        in_specs=[vmem, vmem, vmem],
        out_specs=(anyw, anyw),
        scratch_shapes=[pltpu.VMEM((comps, slots, pts), f32), dma((2,))],
        compiler_params=pltpu.CompilerParams(vmem_limit_bytes=24 * 2**20),
        name="sample_points",
    )(fresh, kvt, held)
    return fresh, sampled.transpose(1, 0, 2)


def solution(mesh):
    return jax.shard_map(
        local,
        mesh=mesh,
        in_specs=(
            P(None, "gz", "gy", None),
            P(("gz", "gy"), None, None),
            P(("gz", "gy"), None, None),
            P(("gz", "gy"), None),
            P(("gz", "gy")),
            P(("gz", "gy")),
        ),
        out_specs=(P(None, "gz", "gy", None), P(("gz", "gy"), None, None)),
        check_vma=False,
    )
```

```python
import functools

import jax
import jax.numpy as jnp
from jax import lax
from jax.experimental import pallas as pl
from jax.experimental.pallas import tpu as pltpu
from jax.sharding import PartitionSpec as P

time_step = 0.25
vmem_bytes = 67043328
viscosity = 0.5
MESH = pl.DeviceIdType.MESH
f32 = jnp.float32
bf16 = jnp.bfloat16


def iota(shape, dim):
    return lax.broadcasted_iota(jnp.int32, shape, dim)


def step_kernel(width, depth, room, vel_hbm, force_hbm, kern_hbm, own_hbm, blk_hbm, cnt_hbm,
                fresh, kvt, held_ref,
                v, kv, force_ref, own_ref, blk_ref, cnt_ref, cells16, edge, hz, pre, left_ref, id_out, id_in, send, recv, back, mine,
                zs, zr, ys, yr,
                in_sem, kern_sem, id_sems, go_sems, re_sems, h_send, h_recv):
    me = lax.axis_index("gy")
    gz = lax.axis_index("gz")
    comps, planes, rows, xcells = v.shape
    _, slots, pts = force_ref.shape
    cells = kv.shape[1]
    nx = xcells // cells
    zy = planes * rows
    total = width * room
    body = comps * cells
    coef = time_step * viscosity
    half = time_step * 0.5
    group = 8
    groups = slots // group
    span = group * pts

    barrier = pltpu.get_barrier_semaphore()
    for k in range(1, width):
        pl.semaphore_signal(barrier, inc=1, device_id={"gy": lax.rem(me + k, width)}, device_id_type=MESH)
    z_lo, z_hi = gz > 0, gz < depth - 1
    y_lo, y_hi = me > 0, me < width - 1

    @pl.when(z_lo)
    def _():
        pl.semaphore_signal(barrier, inc=1, device_id={"gz": gz - 1}, device_id_type=MESH)

    @pl.when(z_hi)
    def _():
        pl.semaphore_signal(barrier, inc=1, device_id={"gz": gz + 1}, device_id_type=MESH)

    inner = pl.ds(1, planes - 2)
    gets = [pltpu.make_async_copy(src, dst, in_sem.at[i]) for i, (src, dst) in enumerate((
        (own_hbm, own_ref), (blk_hbm, blk_ref), (cnt_hbm, cnt_ref), (force_hbm, force_ref),
        (vel_hbm.at[:, 0], v.at[:, 0]), (vel_hbm.at[:, planes - 1], v.at[:, planes - 1]),
        (vel_hbm.at[:, :, 0], edge.at[0]), (vel_hbm.at[:, :, rows - 1], edge.at[1]),
        (vel_hbm.at[:, inner], v.at[:, inner])))]
    halves = 2 if groups % 2 == 0 else 1
    part_rows = groups // halves * span
    get_kern = [pltpu.make_async_copy(kern_hbm.at[pl.ds(h * part_rows, part_rows)],
                                      kv.at[pl.ds(h * part_rows, part_rows)], kern_sem.at[h])
                for h in range(halves)]
    for copy in gets[:8] + get_kern + gets[8:]:
        copy.start()

    for copy in gets[:3]:
        copy.wait()
    rowi, coli = iota((slots, slots), 0), iota((slots, slots), 1)
    own_r = jnp.broadcast_to(own_ref[...].astype(f32), (slots, slots))
    own_c = jnp.sum(jnp.where(rowi == coli, own_r, 0.0), axis=1, keepdims=True)
    same = jnp.where(own_r == own_c, 1.0, 0.0)
    rank_c = jnp.sum(jnp.where(coli < rowi, same, 0.0), axis=1, keepdims=True)
    rank_r = jnp.sum(jnp.where(rowi < coli, same, 0.0), axis=0, keepdims=True)
    count = cnt_ref[...]
    me_f = me.astype(f32)

    def slot_of(owner, rank, index):
        offset = owner - me_f
        offset = jnp.where(offset < 0.0, offset + width, offset)
        return jnp.where(index < count, offset * room + rank, -1.0)

    slot_c = slot_of(own_c, rank_c, iota((slots, 1), 0))
    slot_r = slot_of(own_r[0:1, :], rank_r, iota((1, slots), 1))
    chosen = iota((total, slots), 0).astype(f32) == slot_r
    ids = jnp.sum(jnp.where(chosen, blk_ref[...].astype(f32) + 1.0, 0.0), axis=1, keepdims=True) - 1.0
    slot_lane = iota((room, 128), 1) == iota((room, 128), 0)
    for k in range(width):
        id_out[k] = jnp.sum(jnp.where(slot_lane, ids[k * room:(k + 1) * room], 0.0), axis=0, keepdims=True)

    gets[3].wait()
    line8 = iota((group, pts), 0)
    for g in range(groups):
        for c in range(comps):
            rows_f = force_ref[c, g * group:(g + 1) * group, :].astype(f32)
            for i in range(group):
                left_ref[g, c * group:(c + 1) * group, i * pts:(i + 1) * pts] = jnp.where(
                    line8 == i, rows_f, 0.0).astype(bf16)
    gets[4].wait()
    gets[5].wait()
    for c in range(comps):
        zs[0, c] = v[c, 0].astype(bf16)
        zs[1, c] = v[c, planes - 1].astype(bf16)

    def halo(src, dst, sem, axis, target):
        return pltpu.make_async_remote_copy(
            src_ref=src, dst_ref=dst, send_sem=h_send.at[sem], recv_sem=h_recv.at[sem],
            device_id={axis: target}, device_id_type=MESH)

    z_down = halo(zs.at[0], zr.at[1], 1, "gz", gz - 1)
    z_up = halo(zs.at[1], zr.at[0], 0, "gz", gz + 1)
    y_down = halo(ys.at[0], yr.at[1], 3, "gy", me - 1)
    y_up = halo(ys.at[1], yr.at[0], 2, "gy", me + 1)

    early = me >= width // 2
    late = jnp.logical_not(early)

    def enter():
        pl.semaphore_wait(barrier, width - 1 + z_lo.astype(jnp.int32) + z_hi.astype(jnp.int32))

    def start_z(when):
        for there, copy in ((z_lo, z_down), (z_hi, z_up)):
            pl.when(jnp.logical_and(when, there))(copy.start)

    def start_y(when):
        for there, copy in ((y_lo, y_down), (y_hi, y_up)):
            pl.when(jnp.logical_and(when, there))(copy.start)

    pl.when(early)(enter)
    start_z(early)
    gets[6].wait()
    gets[7].wait()
    ys[...] = edge[...].astype(bf16)
    start_y(early)
    parts = []
    for h in range(halves):
        get_kern[h].wait()
        for g in range(h * groups // halves, (h + 1) * groups // halves):
            parts.append(jnp.dot(left_ref[g], kv[g * span:(g + 1) * span, :], preferred_element_type=f32))
    spread = jnp.concatenate([
        jnp.concatenate([part[c * group:(c + 1) * group] for part in parts], axis=0)
        for c in range(comps)], axis=1).astype(bf16)
    placed = jnp.dot(jnp.where(chosen, 1.0, 0.0).astype(bf16), spread, preferred_element_type=f32)
    send[...] = placed.reshape(width, room, body).astype(bf16)

    pl.when(late)(enter)
    start_z(late)

    after = width - 1 - me
    right = (after >= me).astype(jnp.int32)
    big = right * after + (1 - right) * me
    small = width - 1 - big
    far_first = []
    for j in range(width - 1):
        one = (j < big - small).astype(jnp.int32)
        rest = (1 - one) * (j - big + small)
        step = one * (big - j) + (1 - one) * (small - rest // 2)
        far_first.append(me + (2 * right - 1) * (1 - 2 * (rest % 2)) * step)

    def out(src, dst, sems, targets, back_by=False):
        for target in targets:
            gap = me - target if back_by else target - me
            k = lax.rem(gap + width, width)
            pltpu.make_async_remote_copy(
                src_ref=src.at[k], dst_ref=dst.at[k], send_sem=sems.at[0], recv_sem=sems.at[1],
                device_id={"gy": target}, device_id_type=MESH).start()

    def sent(src, dst, sems):
        rest = pl.ds(1, width - 1)
        return pltpu.make_async_remote_copy(
            src_ref=src.at[rest], dst_ref=dst.at[rest], send_sem=sems.at[0], recv_sem=sems.at[1],
            device_id={"gy": far_first[0]}, device_id_type=MESH)

    out(id_out, id_in, id_sems, far_first)
    out(send, recv, go_sems, far_first[:2])
    start_y(late)
    out(send, recv, go_sems, far_first[2:])
    id_in[0] = id_out[0]
    recv[0] = send[0]

    gets[8].wait()
    lane = iota((rows, xcells), 1)
    line = iota((rows, xcells), 0)
    first_x, last_x = lane == 0, lane == xcells - 1
    first_y, last_y = line == 0, line == rows - 1

    def plane(z, carry):
        vx, vy, vz = v[0, z], v[1, z], v[2, z]
        xu_w = jnp.where(last_x, 0.0, coef - half * vx)
        xd_w = jnp.where(first_x, 0.0, coef + half * vx)
        yu_w = jnp.where(last_y, 0.0, coef - half * vy)
        yd_w = jnp.where(first_y, 0.0, coef + half * vy)
        zu_w = jnp.where(z == planes - 1, 0.0, coef - half * vz)
        zd_w = jnp.where(z == 0, 0.0, coef + half * vz)
        above, below = jnp.minimum(z + 1, planes - 1), jnp.maximum(z - 1, 0)
        for c in range(comps):
            mid = v[c, z]
            value = (1.0 - 6.0 * coef) * mid
            value += xu_w * pltpu.roll(mid, xcells - 1, 1) + xd_w * pltpu.roll(mid, 1, 1)
            value += yu_w * pltpu.roll(mid, rows - 1, 0) + yd_w * pltpu.roll(mid, 1, 0)
            value += zu_w * v[c, above] + zd_w * v[c, below]
            fresh[c, z] = value
        return carry

    lax.fori_loop(0, planes, plane, 0)

    for there, copy, buf, y, sign in ((y_lo, y_up, 0, 0, half), (y_hi, y_down, 1, rows - 1, -half)):
        @pl.when(there)
        def _(copy=copy, buf=buf, y=y, sign=sign):
            copy.wait_recv()
            for c in range(comps):
                got = yr[buf, c].astype(f32)
                for z in range(planes):
                    w = coef + sign * v[1, z, y:y + 1, :]
                    fresh[c, z, y:y + 1, :] += w * got[z:z + 1, :]

    def split(z, carry):
        at = pl.ds(pl.multiple_of(z * rows, rows), rows)
        low = pl.ds(pl.multiple_of(zy + z * rows, rows), rows)
        for c in range(comps):
            value = fresh[c, z]
            high = value.astype(bf16)
            cells16[c, at, :] = high
            cells16[c, low, :] = (value - high.astype(f32)).astype(bf16)
        return carry

    lax.fori_loop(0, planes, split, 0)

    sent(id_out, id_in, id_sems).wait()
    theirs = jnp.concatenate([jnp.broadcast_to(id_in[k], (room, 128)) for k in range(width)], axis=0)
    slot_lane = iota((total, 128), 1) == iota((total, 128), 0) % room
    theirs = jnp.sum(jnp.where(slot_lane, theirs, 0.0), axis=1, keepdims=True)
    place = (iota((total, zy), 1) * nx).astype(f32)
    takes = [jnp.where(place + float(b) == theirs, 1.0, 0.0).astype(bf16) for b in range(nx)]
    column = iota((total, nx * 4 * rows), 1)
    column_row = column % (2 * rows)
    column_row += jnp.where(column_row < rows, 0, zy - 2 * rows)
    column_id = (column_row * nx + column // (4 * rows)).astype(f32)
    ends = jnp.where(column_id == theirs, 1.0, 0.0).astype(bf16)
    every = jnp.concatenate(takes, axis=1)
    match = lax.dot_general(every, every, (((1,), (1,)), ((), ())), preferred_element_type=f32)
    match = (match * time_step).astype(bf16)
    twice = [jnp.concatenate([take, take], axis=1) for take in takes]
    for c in range(comps):
        part = jnp.dot(twice[0], cells16[c, :, :cells], preferred_element_type=f32)
        for b in range(1, nx):
            part += jnp.dot(twice[b], cells16[c, :, b * cells:(b + 1) * cells], preferred_element_type=f32)
        pre[:, c * cells:(c + 1) * cells] = part
    z_sides = ((z_lo, z_up, 0, 0, half), (z_hi, z_down, 1, planes - 1, -half))
    for there, copy, buf, z, sign in z_sides:
        @pl.when(there)
        def _(copy=copy, buf=buf, z=z, sign=sign):
            copy.wait_recv()
            w = coef + sign * v[2, z]
            for c in range(comps):
                value = w * zr[buf, c].astype(f32)
                high = value.astype(bf16)
                low = (value - high.astype(f32)).astype(bf16)
                for b in range(nx):
                    for part, at in ((high, buf * rows), (low, (2 + buf) * rows)):
                        at += b * 4 * rows
                        hz[at:at + rows, c * cells:(c + 1) * cells] = part[:, b * cells:(b + 1) * cells]

        @pl.when(jnp.logical_not(there))
        def _(buf=buf):
            for b in range(nx):
                for at in (buf * rows, (2 + buf) * rows):
                    at += b * 4 * rows
                    hz[at:at + rows, :] = jnp.zeros((rows, body), bf16)

    sent(send, recv, go_sems).wait()
    got = recv[...].astype(f32).reshape(total, body).astype(bf16)
    late_part = jnp.dot(jnp.concatenate([match, ends], axis=1), jnp.concatenate([got, hz[...]], axis=0),
                        preferred_element_type=f32)
    back[...] = (pre[...] + late_part).reshape(width, room, body).astype(bf16)

    out(back, mine, re_sems, far_first, True)
    mine[0] = back[0]

    for there, copy, buf, z, sign in z_sides:
        @pl.when(there)
        def _(buf=buf, z=z, sign=sign):
            w = coef + sign * v[2, z]
            for c in range(comps):
                fresh[c, z] += w * zr[buf, c].astype(f32)

    for b in range(nx):
        put = (takes[b].astype(f32) * time_step).T.astype(bf16)
        part = jnp.dot(put, got, preferred_element_type=f32)
        for c in range(comps):
            where = (c, slice(None), slice(None), slice(b * cells, (b + 1) * cells))
            fresh[where] += part[:, c * cells:(c + 1) * cells].reshape(planes, rows, cells)
    for t in range(slots * pts // cells):
        kvt[:, t * cells:(t + 1) * cells] = kv[t * cells:(t + 1) * cells, :].T
    for there, copy in ((z_lo, z_down), (z_hi, z_up), (y_lo, y_down), (y_hi, y_up)):
        pl.when(there)(copy.wait_send)
    pick = jnp.where(iota((slots, total), 1).astype(f32) == slot_c, 1.0, 0.0).astype(bf16)
    sent(back, mine, re_sems).wait()
    held = mine[...].astype(f32).reshape(total, body).astype(bf16)
    held_ref[...] = jnp.dot(pick, held, preferred_element_type=f32).astype(bf16)


def sample_kernel(fresh, kvt, held_ref, fresh_hbm, out_hbm, out_ref, out_sem):
    comps, slots, pts = out_ref.shape
    cells = kvt.shape[0]
    group = 8
    put_v = pltpu.make_async_copy(fresh, fresh_hbm, out_sem.at[0])
    put_v.start()
    line8 = iota((group, pts), 0)
    for g in range(slots // group):
        part = held_ref[g * group:(g + 1) * group, :].astype(f32)
        left = jnp.concatenate([part[:, c * cells:(c + 1) * cells] for c in range(comps)], axis=0).astype(bf16)
        result = jnp.dot(left, kvt[:, g * group * pts:(g + 1) * group * pts], preferred_element_type=f32)
        for c in range(comps):
            value = jnp.zeros((group, pts), f32)
            for i in range(group):
                value = jnp.where(line8 == i, result[c * group:(c + 1) * group, i * pts:(i + 1) * pts], value)
            out_ref[c, g * group:(g + 1) * group, :] = value
    put_p = pltpu.make_async_copy(out_ref, out_hbm, out_sem.at[1])
    put_p.start()
    put_v.wait()
    put_p.wait()


def local(velocity, forces, kernels, owners, blocks, counts):
    width, depth = lax.axis_size("gy"), lax.axis_size("gz")
    slots, comps, pts = forces.shape
    cells = kernels.shape[2]
    _, planes, rows, xcells = velocity.shape
    room = max(2, (2 * slots + width - 1) // width)
    room = (room + 7) // 8 * 8
    total, body = width * room, comps * cells
    vmem = pl.BlockSpec(memory_space=pltpu.VMEM)
    anyw = pl.BlockSpec(memory_space=pltpu.HBM)
    dma = pltpu.SemaphoreType.DMA
    pair = dma((2,))
    kept = 4 * velocity.size + 2 * kernels.size + 2 * slots * body
    fresh, kvt, held = pl.pallas_call(
        functools.partial(step_kernel, width, depth, room),
        out_shape=(
            pltpu.VMEM(velocity.shape, f32),
            pltpu.VMEM((cells, slots * pts), bf16),
            pltpu.VMEM((slots, body), bf16),
        ),
        in_specs=[anyw] * 6,
        out_specs=(vmem, vmem, vmem),
        scratch_shapes=[
            pltpu.VMEM(velocity.shape, f32),
            pltpu.VMEM((slots * pts, cells), bf16),
            pltpu.VMEM((comps, slots, pts), bf16),
            pltpu.VMEM((1, slots), jnp.int32),
            pltpu.VMEM((1, slots), jnp.int32),
            pltpu.VMEM((1, 1), jnp.int32),
            pltpu.VMEM((comps, 2 * planes * rows, xcells), bf16),
            pltpu.VMEM((2, comps, planes, xcells), f32),
            pltpu.VMEM((xcells // cells * 4 * rows, body), bf16),
            pltpu.VMEM((total, body), f32),
            pltpu.VMEM((slots // 8, comps * 8, 8 * pts), bf16),
            pltpu.VMEM((width, 1, 128), f32),
            pltpu.VMEM((width, 1, 128), f32),
            pltpu.VMEM((width, room, body), bf16),
            pltpu.VMEM((width, room, body), bf16),
            pltpu.VMEM((width, room, body), bf16),
            pltpu.VMEM((width, room, body), bf16),
            pltpu.VMEM((2, comps, rows, xcells), bf16),
            pltpu.VMEM((2, comps, rows, xcells), bf16),
            pltpu.VMEM((2, comps, planes, xcells), bf16),
            pltpu.VMEM((2, comps, planes, xcells), bf16),
            dma((9,)), dma((2,)), pair, pair, pair, dma((4,)), dma((4,)),
        ],
        compiler_params=pltpu.CompilerParams(
            collective_id=0, has_side_effects=True, vmem_limit_bytes=vmem_bytes - kept - 512 * 1024),
        name="boundary_step",
    )(velocity, forces.transpose(1, 0, 2), kernels.reshape(slots * pts, cells),
      owners.reshape(1, slots), blocks.reshape(1, slots), counts.reshape(1, 1))
    fresh, sampled = pl.pallas_call(
        sample_kernel,
        out_shape=(
            jax.ShapeDtypeStruct(velocity.shape, f32),
            jax.ShapeDtypeStruct((comps, slots, pts), f32),
        ),
        in_specs=[vmem, vmem, vmem],
        out_specs=(anyw, anyw),
        scratch_shapes=[pltpu.VMEM((comps, slots, pts), f32), dma((2,))],
        compiler_params=pltpu.CompilerParams(vmem_limit_bytes=24 * 2**20),
        name="sample_points",
    )(fresh, kvt, held)
    return fresh, sampled.transpose(1, 0, 2)


def solution(mesh):
    return jax.shard_map(
        local,
        mesh=mesh,
        in_specs=(
            P(None, "gz", "gy", None),
            P(("gz", "gy"), None, None),
            P(("gz", "gy"), None, None),
            P(("gz", "gy"), None),
            P(("gz", "gy")),
            P(("gz", "gy")),
        ),
        out_specs=(P(None, "gz", "gy", None), P(("gz", "gy"), None, None)),
        check_vma=False,
    )
```

```python
import functools

import jax
import jax.numpy as jnp
from jax import lax
from jax.experimental import pallas as pl
from jax.experimental.pallas import tpu as pltpu
from jax.sharding import PartitionSpec as P

time_step = 0.25
vmem_bytes = 67043328
viscosity = 0.5
MESH = pl.DeviceIdType.MESH
f32 = jnp.float32
bf16 = jnp.bfloat16


def iota(shape, dim):
    return lax.broadcasted_iota(jnp.int32, shape, dim)


def step_kernel(width, depth, room, vel_hbm, force_hbm, kern_hbm, own_hbm, blk_hbm, cnt_hbm,
                fresh, kvt, held_ref,
                v, kv, force_ref, index, cnt_ref, cells16, edge, hz, pre, left_ref, id_out, id_in, send, recv, back, mine,
                zs, zr, ys, yr,
                in_sem, kern_sem, id_sems, go_sems, re_sems, h_send, h_recv):
    me = lax.axis_index("gy")
    gz = lax.axis_index("gz")
    comps, planes, rows, xcells = v.shape
    _, slots, pts = force_ref.shape
    cells = kv.shape[1]
    nx = xcells // cells
    zy = planes * rows
    total = width * room
    body = comps * cells
    coef = time_step * viscosity
    half = time_step * 0.5
    group = 8
    groups = slots // group
    span = group * pts

    barrier = pltpu.get_barrier_semaphore()
    for k in range(1, width):
        pl.semaphore_signal(barrier, inc=1, device_id={"gy": lax.rem(me + k, width)}, device_id_type=MESH)
    z_lo, z_hi = gz > 0, gz < depth - 1
    y_lo, y_hi = me > 0, me < width - 1

    @pl.when(z_lo)
    def _():
        pl.semaphore_signal(barrier, inc=1, device_id={"gz": gz - 1}, device_id_type=MESH)

    @pl.when(z_hi)
    def _():
        pl.semaphore_signal(barrier, inc=1, device_id={"gz": gz + 1}, device_id_type=MESH)

    inner = pl.ds(1, planes - 2)
    gets = [pltpu.make_async_copy(src, dst, in_sem.at[i]) for i, src, dst in (
        (0, own_hbm, index.at[pl.ds(0, 1)]), (0, blk_hbm, index.at[pl.ds(1, 1)]), (1, cnt_hbm, cnt_ref),
        (2, force_hbm, force_ref),
        (3, vel_hbm.at[:, 0], v.at[:, 0]), (3, vel_hbm.at[:, planes - 1], v.at[:, planes - 1]),
        (4, vel_hbm.at[:, :, 0], edge.at[0]), (4, vel_hbm.at[:, :, rows - 1], edge.at[1]),
        (5, vel_hbm.at[:, inner], v.at[:, inner]))]
    both_index = pltpu.make_async_copy(index, index, in_sem.at[0])
    both_planes = pltpu.make_async_copy(v.at[:, pl.ds(0, 2)], v.at[:, pl.ds(0, 2)], in_sem.at[3])
    both_edges = pltpu.make_async_copy(edge, edge, in_sem.at[4])
    halves = 2 if groups % 2 == 0 else 1
    part_rows = groups // halves * span
    get_kern = [pltpu.make_async_copy(kern_hbm.at[pl.ds(h * part_rows, part_rows)],
                                      kv.at[pl.ds(h * part_rows, part_rows)], kern_sem.at[h])
                for h in range(halves)]
    for copy in gets[:8] + get_kern + gets[8:]:
        copy.start()

    both_index.wait()
    gets[2].wait()
    rowi, coli = iota((slots, slots), 0), iota((slots, slots), 1)
    own_r = jnp.broadcast_to(index[0:1, :].astype(f32), (slots, slots))
    own_c = jnp.sum(jnp.where(rowi == coli, own_r, 0.0), axis=1, keepdims=True)
    same = jnp.where(own_r == own_c, 1.0, 0.0)
    rank_c = jnp.sum(jnp.where(coli < rowi, same, 0.0), axis=1, keepdims=True)
    rank_r = jnp.sum(jnp.where(rowi < coli, same, 0.0), axis=0, keepdims=True)
    count = cnt_ref[...]
    me_f = me.astype(f32)

    def slot_of(owner, rank, index):
        offset = owner - me_f
        offset = jnp.where(offset < 0.0, offset + width, offset)
        return jnp.where(index < count, offset * room + rank, -1.0)

    slot_c = slot_of(own_c, rank_c, iota((slots, 1), 0))
    slot_r = slot_of(own_r[0:1, :], rank_r, iota((1, slots), 1))
    chosen = iota((total, slots), 0).astype(f32) == slot_r
    ids = jnp.sum(jnp.where(chosen, index[1:2, :].astype(f32) + 1.0, 0.0), axis=1, keepdims=True) - 1.0
    slot_lane = iota((room, 128), 1) == iota((room, 128), 0)
    for k in range(width):
        id_out[k] = jnp.sum(jnp.where(slot_lane, ids[k * room:(k + 1) * room], 0.0), axis=0, keepdims=True)

    gets[3].wait()
    line8 = iota((group, pts), 0)
    for g in range(groups):
        for c in range(comps):
            rows_f = force_ref[c, g * group:(g + 1) * group, :].astype(f32)
            for i in range(group):
                left_ref[g, c * group:(c + 1) * group, i * pts:(i + 1) * pts] = jnp.where(
                    line8 == i, rows_f, 0.0).astype(bf16)
    both_planes.wait()
    for c in range(comps):
        zs[0, c] = v[c, 0].astype(bf16)
        zs[1, c] = v[c, planes - 1].astype(bf16)

    def halo(src, dst, sem, axis, target):
        return pltpu.make_async_remote_copy(
            src_ref=src, dst_ref=dst, send_sem=h_send.at[sem], recv_sem=h_recv.at[sem],
            device_id={axis: target}, device_id_type=MESH)

    z_down = halo(zs.at[0], zr.at[1], 1, "gz", gz - 1)
    z_up = halo(zs.at[1], zr.at[0], 0, "gz", gz + 1)
    y_down = halo(ys.at[0], yr.at[1], 3, "gy", me - 1)
    y_up = halo(ys.at[1], yr.at[0], 2, "gy", me + 1)

    early = me >= width // 2
    late = jnp.logical_not(early)

    def enter():
        pl.semaphore_wait(barrier, width - 1 + z_lo.astype(jnp.int32) + z_hi.astype(jnp.int32))

    def start_z(when):
        for there, copy in ((z_lo, z_down), (z_hi, z_up)):
            pl.when(jnp.logical_and(when, there))(copy.start)

    def start_y(when):
        for there, copy in ((y_lo, y_down), (y_hi, y_up)):
            pl.when(jnp.logical_and(when, there))(copy.start)

    pl.when(early)(enter)
    start_z(early)
    both_edges.wait()
    ys[...] = edge[...].astype(bf16)
    start_y(early)
    parts = []
    for h in range(halves):
        get_kern[h].wait()
        for g in range(h * groups // halves, (h + 1) * groups // halves):
            parts.append(jnp.dot(left_ref[g], kv[g * span:(g + 1) * span, :], preferred_element_type=f32))
    spread = jnp.concatenate([
        jnp.concatenate([part[c * group:(c + 1) * group] for part in parts], axis=0)
        for c in range(comps)], axis=1).astype(bf16)
    placed = jnp.dot(jnp.where(chosen, 1.0, 0.0).astype(bf16), spread, preferred_element_type=f32)
    send[...] = placed.reshape(width, room, body).astype(bf16)

    pl.when(late)(enter)
    start_z(late)

    after = width - 1 - me
    right = (after >= me).astype(jnp.int32)
    big = right * after + (1 - right) * me
    small = width - 1 - big
    far_first = []
    for j in range(width - 1):
        one = (j < big - small).astype(jnp.int32)
        rest = (1 - one) * (j - big + small)
        step = one * (big - j) + (1 - one) * (small - rest // 2)
        far_first.append(me + (2 * right - 1) * (1 - 2 * (rest % 2)) * step)

    def out(src, dst, sems, targets, back_by=False):
        for target in targets:
            gap = me - target if back_by else target - me
            k = lax.rem(gap + width, width)
            pltpu.make_async_remote_copy(
                src_ref=src.at[k], dst_ref=dst.at[k], send_sem=sems.at[0], recv_sem=sems.at[1],
                device_id={"gy": target}, device_id_type=MESH).start()

    def sent(src, dst, sems):
        rest = pl.ds(1, width - 1)
        return pltpu.make_async_remote_copy(
            src_ref=src.at[rest], dst_ref=dst.at[rest], send_sem=sems.at[0], recv_sem=sems.at[1],
            device_id={"gy": far_first[0]}, device_id_type=MESH)

    out(id_out, id_in, id_sems, far_first)
    out(send, recv, go_sems, far_first[:2])
    start_y(late)
    out(send, recv, go_sems, far_first[2:])
    id_in[0] = id_out[0]
    recv[0] = send[0]

    gets[8].wait()
    lane = iota((rows, xcells), 1)
    line = iota((rows, xcells), 0)
    first_x, last_x = lane == 0, lane == xcells - 1
    first_y, last_y = line == 0, line == rows - 1

    def plane(z, carry):
        vx, vy, vz = v[0, z], v[1, z], v[2, z]
        xu_w = jnp.where(last_x, 0.0, coef - half * vx)
        xd_w = jnp.where(first_x, 0.0, coef + half * vx)
        yu_w = jnp.where(last_y, 0.0, coef - half * vy)
        yd_w = jnp.where(first_y, 0.0, coef + half * vy)
        zu_w = jnp.where(z == planes - 1, 0.0, coef - half * vz)
        zd_w = jnp.where(z == 0, 0.0, coef + half * vz)
        above, below = jnp.minimum(z + 1, planes - 1), jnp.maximum(z - 1, 0)
        for c in range(comps):
            mid = v[c, z]
            value = (1.0 - 6.0 * coef) * mid
            value += xu_w * pltpu.roll(mid, xcells - 1, 1) + xd_w * pltpu.roll(mid, 1, 1)
            value += yu_w * pltpu.roll(mid, rows - 1, 0) + yd_w * pltpu.roll(mid, 1, 0)
            value += zu_w * v[c, above] + zd_w * v[c, below]
            fresh[c, z] = value
        return carry

    lax.fori_loop(0, planes, plane, 0)

    for there, copy, buf, y, sign in ((y_lo, y_up, 0, 0, half), (y_hi, y_down, 1, rows - 1, -half)):
        @pl.when(there)
        def _(copy=copy, buf=buf, y=y, sign=sign):
            copy.wait_recv()
            for c in range(comps):
                got = yr[buf, c].astype(f32)
                for z in range(planes):
                    w = coef + sign * v[1, z, y:y + 1, :]
                    fresh[c, z, y:y + 1, :] += w * got[z:z + 1, :]

    def split(z, carry):
        at = pl.ds(pl.multiple_of(z * rows, rows), rows)
        low = pl.ds(pl.multiple_of(zy + z * rows, rows), rows)
        for c in range(comps):
            value = fresh[c, z]
            high = value.astype(bf16)
            cells16[c, at, :] = high
            cells16[c, low, :] = (value - high.astype(f32)).astype(bf16)
        return carry

    lax.fori_loop(0, planes, split, 0)

    sent(id_out, id_in, id_sems).wait()
    theirs = jnp.concatenate([jnp.broadcast_to(id_in[k], (room, 128)) for k in range(width)], axis=0)
    slot_lane = iota((total, 128), 1) == iota((total, 128), 0) % room
    theirs = jnp.sum(jnp.where(slot_lane, theirs, 0.0), axis=1, keepdims=True)
    place = (iota((total, zy), 1) * nx).astype(f32)
    takes = [jnp.where(place + float(b) == theirs, 1.0, 0.0).astype(bf16) for b in range(nx)]
    column = iota((total, nx * 4 * rows), 1)
    column_row = column % (2 * rows)
    column_row += jnp.where(column_row < rows, 0, zy - 2 * rows)
    column_id = (column_row * nx + column // (4 * rows)).astype(f32)
    ends = jnp.where(column_id == theirs, 1.0, 0.0).astype(bf16)
    every = jnp.concatenate(takes, axis=1)
    match = lax.dot_general(every, every, (((1,), (1,)), ((), ())), preferred_element_type=f32)
    match = (match * time_step).astype(bf16)
    twice = [jnp.concatenate([take, take], axis=1) for take in takes]
    for c in range(comps):
        part = jnp.dot(twice[0], cells16[c, :, :cells], preferred_element_type=f32)
        for b in range(1, nx):
            part += jnp.dot(twice[b], cells16[c, :, b * cells:(b + 1) * cells], preferred_element_type=f32)
        pre[:, c * cells:(c + 1) * cells] = part
    z_sides = ((z_lo, z_up, 0, 0, half), (z_hi, z_down, 1, planes - 1, -half))
    for there, copy, buf, z, sign in z_sides:
        @pl.when(there)
        def _(copy=copy, buf=buf, z=z, sign=sign):
            copy.wait_recv()
            w = coef + sign * v[2, z]
            for c in range(comps):
                value = w * zr[buf, c].astype(f32)
                high = value.astype(bf16)
                low = (value - high.astype(f32)).astype(bf16)
                for b in range(nx):
                    for part, at in ((high, buf * rows), (low, (2 + buf) * rows)):
                        at += b * 4 * rows
                        hz[at:at + rows, c * cells:(c + 1) * cells] = part[:, b * cells:(b + 1) * cells]

        @pl.when(jnp.logical_not(there))
        def _(buf=buf):
            for b in range(nx):
                for at in (buf * rows, (2 + buf) * rows):
                    at += b * 4 * rows
                    hz[at:at + rows, :] = jnp.zeros((rows, body), bf16)

    sent(send, recv, go_sems).wait()
    got = recv[...].astype(f32).reshape(total, body).astype(bf16)
    late_part = jnp.dot(jnp.concatenate([match, ends], axis=1), jnp.concatenate([got, hz[...]], axis=0),
                        preferred_element_type=f32)
    back[...] = (pre[...] + late_part).reshape(width, room, body).astype(bf16)

    out(back, mine, re_sems, far_first, True)
    mine[0] = back[0]

    for there, copy, buf, z, sign in z_sides:
        @pl.when(there)
        def _(buf=buf, z=z, sign=sign):
            w = coef + sign * v[2, z]
            for c in range(comps):
                fresh[c, z] += w * zr[buf, c].astype(f32)

    for b in range(nx):
        put = (takes[b].astype(f32) * time_step).T.astype(bf16)
        part = jnp.dot(put, got, preferred_element_type=f32)
        for c in range(comps):
            where = (c, slice(None), slice(None), slice(b * cells, (b + 1) * cells))
            fresh[where] += part[:, c * cells:(c + 1) * cells].reshape(planes, rows, cells)
    for t in range(slots * pts // cells):
        kvt[:, t * cells:(t + 1) * cells] = kv[t * cells:(t + 1) * cells, :].T
    for there, copy in ((z_lo, z_down), (z_hi, z_up), (y_lo, y_down), (y_hi, y_up)):
        pl.when(there)(copy.wait_send)
    pick = jnp.where(iota((slots, total), 1).astype(f32) == slot_c, 1.0, 0.0).astype(bf16)
    sent(back, mine, re_sems).wait()
    held = mine[...].astype(f32).reshape(total, body).astype(bf16)
    held_ref[...] = jnp.dot(pick, held, preferred_element_type=f32).astype(bf16)


def sample_kernel(fresh, kvt, held_ref, fresh_hbm, out_hbm, out_ref, out_sem):
    comps, slots, pts = out_ref.shape
    cells = kvt.shape[0]
    group = 8
    put_v = pltpu.make_async_copy(fresh, fresh_hbm, out_sem.at[0])
    put_v.start()
    line8 = iota((group, pts), 0)
    for g in range(slots // group):
        part = held_ref[g * group:(g + 1) * group, :].astype(f32)
        left = jnp.concatenate([part[:, c * cells:(c + 1) * cells] for c in range(comps)], axis=0).astype(bf16)
        result = jnp.dot(left, kvt[:, g * group * pts:(g + 1) * group * pts], preferred_element_type=f32)
        for c in range(comps):
            value = jnp.zeros((group, pts), f32)
            for i in range(group):
                value = jnp.where(line8 == i, result[c * group:(c + 1) * group, i * pts:(i + 1) * pts], value)
            out_ref[c, g * group:(g + 1) * group, :] = value
    put_p = pltpu.make_async_copy(out_ref, out_hbm, out_sem.at[1])
    put_p.start()
    put_v.wait()
    put_p.wait()


def local(velocity, forces, kernels, owners, blocks, counts):
    width, depth = lax.axis_size("gy"), lax.axis_size("gz")
    slots, comps, pts = forces.shape
    cells = kernels.shape[2]
    _, planes, rows, xcells = velocity.shape
    room = max(2, (2 * slots + width - 1) // width)
    room = (room + 7) // 8 * 8
    total, body = width * room, comps * cells
    vmem = pl.BlockSpec(memory_space=pltpu.VMEM)
    anyw = pl.BlockSpec(memory_space=pltpu.HBM)
    dma = pltpu.SemaphoreType.DMA
    pair = dma((2,))
    kept = 4 * velocity.size + 2 * kernels.size + 2 * slots * body
    fresh, kvt, held = pl.pallas_call(
        functools.partial(step_kernel, width, depth, room),
        out_shape=(
            pltpu.VMEM(velocity.shape, f32),
            pltpu.VMEM((cells, slots * pts), bf16),
            pltpu.VMEM((slots, body), bf16),
        ),
        in_specs=[anyw] * 6,
        out_specs=(vmem, vmem, vmem),
        scratch_shapes=[
            pltpu.VMEM(velocity.shape, f32),
            pltpu.VMEM((slots * pts, cells), bf16),
            pltpu.VMEM((comps, slots, pts), bf16),
            pltpu.VMEM((2, slots), jnp.int32),
            pltpu.VMEM((1, 1), jnp.int32),
            pltpu.VMEM((comps, 2 * planes * rows, xcells), bf16),
            pltpu.VMEM((2, comps, planes, xcells), f32),
            pltpu.VMEM((xcells // cells * 4 * rows, body), bf16),
            pltpu.VMEM((total, body), f32),
            pltpu.VMEM((slots // 8, comps * 8, 8 * pts), bf16),
            pltpu.VMEM((width, 1, 128), f32),
            pltpu.VMEM((width, 1, 128), f32),
            pltpu.VMEM((width, room, body), bf16),
            pltpu.VMEM((width, room, body), bf16),
            pltpu.VMEM((width, room, body), bf16),
            pltpu.VMEM((width, room, body), bf16),
            pltpu.VMEM((2, comps, rows, xcells), bf16),
            pltpu.VMEM((2, comps, rows, xcells), bf16),
            pltpu.VMEM((2, comps, planes, xcells), bf16),
            pltpu.VMEM((2, comps, planes, xcells), bf16),
            dma((6,)), dma((2,)), pair, pair, pair, dma((4,)), dma((4,)),
        ],
        compiler_params=pltpu.CompilerParams(
            collective_id=0, has_side_effects=True, vmem_limit_bytes=vmem_bytes - kept - 512 * 1024),
        name="boundary_step",
    )(velocity, forces.transpose(1, 0, 2), kernels.reshape(slots * pts, cells),
      owners.reshape(1, slots), blocks.reshape(1, slots), counts.reshape(1, 1))
    fresh, sampled = pl.pallas_call(
        sample_kernel,
        out_shape=(
            jax.ShapeDtypeStruct(velocity.shape, f32),
            jax.ShapeDtypeStruct((comps, slots, pts), f32),
        ),
        in_specs=[vmem, vmem, vmem],
        out_specs=(anyw, anyw),
        scratch_shapes=[pltpu.VMEM((comps, slots, pts), f32), dma((2,))],
        compiler_params=pltpu.CompilerParams(vmem_limit_bytes=24 * 2**20),
        name="sample_points",
    )(fresh, kvt, held)
    return fresh, sampled.transpose(1, 0, 2)


def solution(mesh):
    return jax.shard_map(
        local,
        mesh=mesh,
        in_specs=(
            P(None, "gz", "gy", None),
            P(("gz", "gy"), None, None),
            P(("gz", "gy"), None, None),
            P(("gz", "gy"), None),
            P(("gz", "gy")),
            P(("gz", "gy")),
        ),
        out_specs=(P(None, "gz", "gy", None), P(("gz", "gy"), None, None)),
        check_vma=False,
    )
```
